8 devices in a mesh: rep: 2 (over z, y), fsdp: 4 (over x, core).
Axes of the slice: x: 2, y: 2, z: 1, core: 2. Of those that a mesh axis runs over, the one named last changes fastest.
Arguments:
- tok_ids: int32 [8, 256], P(('rep', 'fsdp'))
- tok_labels: int32 [8, 256], P(('rep', 'fsdp'))
- tok_pos: int32 [8, 256], P(('rep', 'fsdp'))
- expert_idx: int32 [2, 8, 256, 2], P(None, ('rep', 'fsdp'))
- learn_rate: float32 [], replicated
- embedding: float32 [32000, 512], P('fsdp')
- w_query: float32 [2, 512, 512], P(None, 'fsdp')
- w_key: float32 [2, 512, 128], P(None, 'fsdp')
- w_value: float32 [2, 512, 128], P(None, 'fsdp')
- w_attn_out: float32 [2, 512, 512], P(None, 'fsdp')
- g_attn: float32 [2, 512], P(None, 'fsdp')
- g_mlp: float32 [2, 512], P(None, 'fsdp')
- w_router: float32 [2, 512, 8], P(None, 'fsdp')
- w_gate: float32 [2, 8, 512, 1792], P(None, None, 'fsdp')
- w_up: float32 [2, 8, 512, 1792], P(None, None, 'fsdp')
- w_down: float32 [2, 8, 1792, 512], P(None, None, 'fsdp')
- g_final: float32 [512], P('fsdp')
- w_head: float32 [512, 32000], P('fsdp')
Outputs:
- output 1: float32 [32000, 512], P('fsdp')
- output 2: float32 [2, 512, 512], P(None, 'fsdp')
- output 3: float32 [2, 512, 128], P(None, 'fsdp')
- output 4: float32 [2, 512, 128], P(None, 'fsdp')
- output 5: float32 [2, 512, 512], P(None, 'fsdp')
- output 6: float32 [2, 512], P(None, 'fsdp')
- output 7: float32 [2, 512], P(None, 'fsdp')
- output 8: float32 [2, 512, 8], P(None, 'fsdp')
- output 9: float32 [2, 8, 512, 1792], P(None, None, 'fsdp')
- output 10: float32 [2, 8, 512, 1792], P(None, None, 'fsdp')
- output 11: float32 [2, 8, 1792, 512], P(None, None, 'fsdp')
- output 12: float32 [512], P('fsdp')
- output 13: float32 [512, 32000], P('fsdp')
- output 14: float32 [], replicated
All inputs are finite; a program needn't handle non-finite values.
Results may differ from the reference program's by a relative error of at most 0.00855285.
Values are sent between devices in bfloat16 or wider.
A program may use at most 1 GiB of HBM per device.

```python
import functools
import jax
import jax.numpy as jnp
from jax import lax

DIM_MODEL = 512
DIM_FF = 1792
Q_HEADS = 4
KV_HEADS = 1
HEAD_DIM = 128
EXPERTS = 8
VOCAB_SIZE = 32000
BATCH_DEV = 1
SEQ_LEN = 256
BATCH_ALL = 8
LAYERS = 2
ROPE_THETA = 1000000.0
NORM_EPS = 1e-5
TOKEN_TOTAL = BATCH_ALL * SEQ_LEN
GROUP_COUNT = BATCH_ALL // BATCH_DEV


def setup_inputs(seed: int = 0) -> dict:
    keys = jax.random.split(jax.random.key(seed), 20)
    tok_shape = (BATCH_ALL, SEQ_LEN)
    route_shape = (LAYERS, BATCH_ALL, SEQ_LEN)
    q_width = Q_HEADS * HEAD_DIM
    kv_width = KV_HEADS * HEAD_DIM

    def normal(key, shape, scale):
        return jax.random.normal(key, shape, jnp.float32) * scale

    tok_ids = jax.random.randint(keys[0], tok_shape, 0, VOCAB_SIZE, dtype=jnp.int32)
    tok_labels = jax.random.randint(keys[1], tok_shape, 0, VOCAB_SIZE, dtype=jnp.int32)
    gaps = jax.random.randint(keys[2], tok_shape, 1, 4, dtype=jnp.int32)
    tok_pos = jnp.cumsum(gaps, axis=1) - gaps[:, :1]
    pick_a = jax.random.randint(keys[3], route_shape, 0, EXPERTS, dtype=jnp.int32)
    pick_b = jax.random.randint(keys[4], route_shape, 0, EXPERTS, dtype=jnp.int32)
    layer_odd = (jnp.arange(LAYERS, dtype=jnp.int32) % 2)[:, None, None]
    first = jnp.where(layer_odd == 0, jnp.minimum(pick_a, pick_b), jnp.maximum(pick_a, pick_b))
    shift = jax.random.randint(keys[5], route_shape, 1, EXPERTS, dtype=jnp.int32)
    second = (first + shift) % EXPERTS
    expert_idx = jnp.stack([first, second], axis=-1)
    learn_rate = (0.15 * TOKEN_TOTAL ** 0.5) * 2.0 ** jax.random.uniform(keys[6], (), jnp.float32, -1.0, 1.0)
    return {
        'tok_ids': tok_ids,
        'tok_labels': tok_labels,
        'tok_pos': tok_pos,
        'expert_idx': expert_idx,
        'learn_rate': learn_rate,
        'embedding': normal(keys[7], (VOCAB_SIZE, DIM_MODEL), 1.0),
        'w_query': normal(keys[8], (LAYERS, DIM_MODEL, q_width), DIM_MODEL ** -0.5),
        'w_key': normal(keys[9], (LAYERS, DIM_MODEL, kv_width), DIM_MODEL ** -0.5),
        'w_value': normal(keys[10], (LAYERS, DIM_MODEL, kv_width), DIM_MODEL ** -0.5),
        'w_attn_out': normal(keys[11], (LAYERS, q_width, DIM_MODEL), q_width ** -0.5),
        'g_attn': 1.0 + normal(keys[12], (LAYERS, DIM_MODEL), 0.3),
        'g_mlp': 1.0 + normal(keys[13], (LAYERS, DIM_MODEL), 0.3),
        'w_router': normal(keys[14], (LAYERS, DIM_MODEL, EXPERTS), DIM_MODEL ** -0.5),
        'w_gate': normal(keys[15], (LAYERS, EXPERTS, DIM_MODEL, DIM_FF), DIM_MODEL ** -0.5),
        'w_up': normal(keys[16], (LAYERS, EXPERTS, DIM_MODEL, DIM_FF), DIM_MODEL ** -0.5),
        'w_down': normal(keys[17], (LAYERS, EXPERTS, DIM_FF, DIM_MODEL), DIM_FF ** -0.5),
        'g_final': 1.0 + normal(keys[18], (DIM_MODEL,), 0.3),
        'w_head': normal(keys[19], (DIM_MODEL, VOCAB_SIZE), DIM_MODEL ** -0.5),
    }


def rms_norm(residual, gain):
    mean_sq = jnp.mean(residual * residual, axis=-1, keepdims=True)
    return (residual * lax.rsqrt(mean_sq + NORM_EPS) * gain.astype(jnp.bfloat16)).astype(jnp.bfloat16)


def rope_tables(positions):
    inv_freq = ROPE_THETA ** (-jnp.arange(0, HEAD_DIM, 2, dtype=jnp.float32) / HEAD_DIM)
    angle = positions.astype(jnp.float32)[..., None] * inv_freq
    return jnp.cos(angle)[:, :, None, :], jnp.sin(angle)[:, :, None, :]


def apply_rope(heads, cos_tab, sin_tab):
    half_dim = heads.shape[-1] // 2
    lower = heads[..., :half_dim]
    upper = heads[..., half_dim:]
    return jnp.concatenate([lower * cos_tab - upper * sin_tab, upper * cos_tab + lower * sin_tab], axis=-1)


def attention_block(normed, w_q, w_k, w_v, w_o, cos_tab, sin_tab):
    batch = normed.shape[0]
    length = normed.shape[1]
    group = Q_HEADS // KV_HEADS
    flat = normed.reshape(batch * length, DIM_MODEL)
    query = jnp.dot(flat, w_q.astype(jnp.bfloat16), preferred_element_type=jnp.float32).reshape(batch, length, Q_HEADS, HEAD_DIM)
    keyed = jnp.dot(flat, w_k.astype(jnp.bfloat16), preferred_element_type=jnp.float32).reshape(batch, length, KV_HEADS, HEAD_DIM)
    values = jnp.dot(flat, w_v.astype(jnp.bfloat16), preferred_element_type=jnp.float32).astype(jnp.bfloat16).reshape(batch, length, KV_HEADS, HEAD_DIM)
    query = apply_rope(query, cos_tab, sin_tab).astype(jnp.bfloat16).reshape(batch, length, KV_HEADS, group, HEAD_DIM)
    keyed = apply_rope(keyed, cos_tab, sin_tab).astype(jnp.bfloat16)
    scores = jnp.einsum('bqkgd,bskd->bkgqs', query.astype(jnp.float32), keyed.astype(jnp.float32)) * HEAD_DIM ** -0.5
    causal = jnp.arange(length)[:, None] >= jnp.arange(length)[None, :]
    scores = jnp.where(causal, scores, -1e30)
    attn_probs = jax.nn.softmax(scores, axis=-1).astype(jnp.bfloat16)
    mixed = jnp.einsum('bkgqs,bskd->bqkgd', attn_probs.astype(jnp.float32), values.astype(jnp.float32)).astype(jnp.bfloat16)
    mixed = mixed.reshape(batch * length, Q_HEADS * HEAD_DIM)
    projected = jnp.dot(mixed, w_o.astype(jnp.bfloat16), preferred_element_type=jnp.float32)
    return projected.reshape(batch, length, DIM_MODEL)


def moe_block(normed, w_r, w_gate, w_up, w_down, chosen):
    batch = normed.shape[0]
    length = normed.shape[1]
    flat = normed.reshape(batch * length, DIM_MODEL)
    chosen_flat = chosen.reshape(batch * length, 2)
    logits = jnp.dot(flat, w_r.astype(jnp.bfloat16), preferred_element_type=jnp.float32)
    gates = jax.nn.softmax(jnp.take_along_axis(logits, chosen_flat, axis=1), axis=-1)
    onehot = (chosen_flat[:, :, None] == jnp.arange(EXPERTS)[None, None, :]).astype(jnp.float32)
    combine = jnp.sum(gates[:, :, None] * onehot, axis=1)
    flat_wide = flat.astype(jnp.float32)
    up_a = jnp.einsum('td,xdf->xtf', flat_wide, w_gate.astype(jnp.bfloat16).astype(jnp.float32))
    up_b = jnp.einsum('td,xdf->xtf', flat_wide, w_up.astype(jnp.bfloat16).astype(jnp.float32))
    hidden = (jax.nn.silu(up_a) * up_b).astype(jnp.bfloat16)
    down = jnp.einsum('xtf,xfd->xtd', hidden.astype(jnp.float32), w_down.astype(jnp.bfloat16).astype(jnp.float32))
    mixed = jnp.einsum('tx,xtd->td', combine, down)
    return mixed.reshape(batch, length, DIM_MODEL)


def group_loss(params, group_inputs):
    ids_grp, labels_grp, pos_grp, route_grp = group_inputs
    (embedding, w_query, w_key, w_value, w_attn_out, g_attn, g_mlp, w_router, w_gate, w_up, w_down, g_final, w_head) = params
    cos_tab, sin_tab = rope_tables(pos_grp)
    residual = jnp.take(embedding.astype(jnp.bfloat16), ids_grp, axis=0).astype(jnp.float32)
    for layer in range(LAYERS):
        normed = rms_norm(residual, g_attn[layer])
        residual = residual + attention_block(normed, w_query[layer], w_key[layer], w_value[layer], w_attn_out[layer], cos_tab, sin_tab)
        normed = rms_norm(residual, g_mlp[layer])
        residual = residual + moe_block(normed, w_router[layer], w_gate[layer], w_up[layer], w_down[layer], route_grp[layer])
    final = rms_norm(residual, g_final).reshape(-1, DIM_MODEL)
    logits = jnp.dot(final, w_head.astype(jnp.bfloat16), preferred_element_type=jnp.float32)
    picked = jnp.take_along_axis(logits, labels_grp.reshape(-1, 1), axis=1)[:, 0]
    return jnp.sum(jax.nn.logsumexp(logits, axis=-1) - picked)


def reference(tok_ids, tok_labels, tok_pos, expert_idx, learn_rate, embedding, w_query, w_key, w_value, w_attn_out, g_attn, g_mlp, w_router, w_gate, w_up, w_down, g_final, w_head):
    params = (embedding, w_query, w_key, w_value, w_attn_out, g_attn, g_mlp, w_router, w_gate, w_up, w_down, g_final, w_head)
    grouped = (
        tok_ids.reshape(GROUP_COUNT, BATCH_DEV, SEQ_LEN),
        tok_labels.reshape(GROUP_COUNT, BATCH_DEV, SEQ_LEN),
        tok_pos.reshape(GROUP_COUNT, BATCH_DEV, SEQ_LEN),
        jnp.moveaxis(expert_idx.reshape(LAYERS, GROUP_COUNT, BATCH_DEV, SEQ_LEN, 2), 1, 0),
    )

    def total_loss(param_tuple):
        body = jax.checkpoint(functools.partial(group_loss, param_tuple))
        return jnp.sum(lax.map(body, grouped)) / TOKEN_TOTAL

    mean_loss, grads = jax.value_and_grad(total_loss)(params)
    updated = [master - learn_rate * gradient for master, gradient in zip(params, grads)]
    return (updated[0], updated[1], updated[2], updated[3], updated[4], updated[5], updated[6], updated[7], updated[8], updated[9], updated[10], updated[11], updated[12], mean_loss)
```

```python
import functools
import jax
import jax.numpy as jnp
from jax import lax
from jax.experimental import pallas as pl
from jax.experimental.pallas import tpu as pltpu
from jax.experimental.layout import Layout, with_layout_constraint
from jax.sharding import PartitionSpec as P

HEAD_DIM = 128
ROPE_THETA = 1000000.0
NORM_EPS = 1e-5
BF16 = jnp.bfloat16
F32 = jnp.float32
VMEM_LIMIT = 60 * 1024 * 1024
FSDP = 'fsdp'
REP = 'rep'


def rms_norm(residual, gain):
    mean_sq = jnp.mean(residual * residual, axis=-1, keepdims=True)
    return (residual * lax.rsqrt(mean_sq + NORM_EPS) * gain).astype(BF16)


def rope_tables(positions):
    inv_freq = ROPE_THETA ** (-jnp.arange(0, HEAD_DIM, 2, dtype=F32) / HEAD_DIM)
    angle = positions.astype(F32)[..., None] * inv_freq
    return jnp.cos(angle)[:, None, :], jnp.sin(angle)[:, None, :]


def apply_rope(heads, cos_tab, sin_tab):
    half_dim = heads.shape[-1] // 2
    lower = heads[..., :half_dim]
    upper = heads[..., half_dim:]
    return jnp.concatenate([lower * cos_tab - upper * sin_tab, upper * cos_tab + lower * sin_tab], axis=-1)


def attention_part(residual, w_q, w_k, w_v, w_o, gain, cos_tab, sin_tab):
    length = residual.shape[0]
    q_heads = w_q.shape[1] // HEAD_DIM
    normed = rms_norm(residual, gain)
    query = jnp.dot(normed, w_q, preferred_element_type=F32).reshape(length, q_heads, HEAD_DIM)
    keyed = jnp.dot(normed, w_k, preferred_element_type=F32).reshape(length, 1, HEAD_DIM)
    values = jnp.dot(normed, w_v, preferred_element_type=F32).astype(BF16)
    query = apply_rope(query, cos_tab, sin_tab).astype(BF16)
    keyed = apply_rope(keyed, cos_tab, sin_tab).astype(BF16)[:, 0]
    scores = jnp.einsum('qgd,sd->gqs', query, keyed, preferred_element_type=F32) * HEAD_DIM ** -0.5
    causal = lax.broadcasted_iota(jnp.int32, (length, length), 0) >= lax.broadcasted_iota(jnp.int32, (length, length), 1)
    scores = jnp.where(causal, scores, -1e30)
    attn_probs = jax.nn.softmax(scores, axis=-1).astype(BF16)
    mixed = jnp.einsum('gqs,sd->qgd', attn_probs, values, preferred_element_type=F32).astype(BF16)
    mixed = mixed.reshape(length, q_heads * HEAD_DIM)
    return residual + jnp.dot(mixed, w_o, preferred_element_type=F32)


def combine_weights(logits, chosen):
    rows = lax.broadcasted_iota(jnp.int32, logits.shape, 0)
    first = rows == chosen[:1]
    second = rows == chosen[1:]
    r0 = jnp.sum(jnp.where(first, logits, 0.0), axis=0, keepdims=True)
    r1 = jnp.sum(jnp.where(second, logits, 0.0), axis=0, keepdims=True)
    gates = jax.nn.softmax(jnp.concatenate([r0, r1], axis=0), axis=0)
    return jnp.where(first, gates[:1], 0.0) + jnp.where(second, gates[1:], 0.0)


def router_logits(normed, w_r):
    return lax.dot_general(w_r, normed, (((0,), (1,)), ((), ())), preferred_element_type=F32)


def router_part(residual, gain, w_r, chosen):
    normed = rms_norm(residual, gain)
    return normed, combine_weights(router_logits(normed, w_r), chosen)


def dot_nn(a, b):
    return jnp.dot(a, b, preferred_element_type=F32)


def dot_nt(a, b):
    return lax.dot_general(a, b, (((1,), (1,)), ((), ())), preferred_element_type=F32)


def params(steps):
    return pltpu.CompilerParams(dimension_semantics=("arbitrary",) * steps, vmem_limit_bytes=VMEM_LIMIT)


def permuted_columns(ref, me):
    return jnp.concatenate([ref[:, pl.ds(pl.multiple_of((me ^ k) * 128, 128), 128)] for k in range(4)], axis=1)


def pack_experts_kernel(sc, gate1, up1, gate2, up2, gate3, up3, down1, out1, out2, out3, out_down):
    rep = sc[2]
    out1[0, 0] = gate1[0, 0].astype(BF16)
    out1[1, 0] = up1[0, 0].astype(BF16)
    out2[0] = jnp.where(rep == 0, gate2[0, 0], up2[0, 0]).astype(BF16)
    out3[0] = jnp.where(rep == 0, gate3[0, 0], up3[0, 0]).astype(BF16)
    out_down[0] = down1[0, 0].astype(BF16)


def pack_experts(sc, layer, w_gate, w_up, w_down):
    def spec(own_core, own_half, matrix=None):
        def index(j, sc):
            step = j if matrix is None else jnp.where(sc[2] == matrix, j, 0)
            core = sc[0] if own_core else 1 - sc[0]
            return layer, 2 * step + core, 0, (sc[1] if own_half else 1 - sc[1])

        return pl.BlockSpec((1, 1, 128, 896), index)

    block = lambda j, sc: (j, 0, 0)
    return pl.pallas_call(
        pack_experts_kernel,
        grid_spec=pltpu.PrefetchScalarGridSpec(
            num_scalar_prefetch=1,
            grid=(4,),
            in_specs=[spec(False, True), spec(False, True), spec(True, False, 0), spec(True, False, 1), spec(False, False, 0), spec(False, False, 1),
                      pl.BlockSpec((1, 1, 448, 512), lambda j, sc: (layer, 2 * j + 1 - sc[0], 0, 0))],
            out_specs=[pl.BlockSpec((2, 1, 128, 896), lambda j, sc: (0, j, 0, 0)), pl.BlockSpec((1, 128, 896), block), pl.BlockSpec((1, 128, 896), block),
                       pl.BlockSpec((1, 448, 512), block)],
        ),
        out_shape=[
            jax.ShapeDtypeStruct((2, 4, 128, 896), BF16),
            jax.ShapeDtypeStruct((4, 128, 896), BF16),
            jax.ShapeDtypeStruct((4, 128, 896), BF16),
            jax.ShapeDtypeStruct((4, 448, 512), BF16),
        ],
        compiler_params=params(1),
        cost_estimate=pl.CostEstimate(flops=10_000_000, bytes_accessed=17_000_000, transcendentals=0),
    )(sc, w_gate, w_up, w_gate, w_up, w_gate, w_up, w_down)


def pack_head_kernel(sc, w_ref, out0, out1, out2, out3):
    core, x, rep = sc[0], sc[1], sc[2]

    def part(xx, cc):
        return w_ref[:, pl.ds(pl.multiple_of(head_start(xx, cc), 128), HEAD_COLS)].astype(BF16)

    out0[...] = part(x, core)
    out1[...] = part(x, 1 - core)

    @pl.when(pl.program_id(0) // (pl.num_programs(0) // 2) == rep)
    def _():
        out2[...] = part(1 - x, core)
        out3[...] = part(1 - x, 1 - core)


def pack_head(sc, w):
    rows, vocab = w.shape
    step = 16
    count = rows // step
    half = lambda i, sc: (jnp.clip(i - sc[2] * (count // 2), 0, count // 2 - 1), 0)
    return pl.pallas_call(
        pack_head_kernel,
        grid_spec=pltpu.PrefetchScalarGridSpec(
            num_scalar_prefetch=1,
            grid=(count,),
            in_specs=[pl.BlockSpec((step, vocab), lambda i, sc: (i, 0))],
            out_specs=[pl.BlockSpec((step, HEAD_COLS), lambda i, sc: (i, 0))] * 2 + [pl.BlockSpec((step, HEAD_COLS), half)] * 2,
        ),
        out_shape=[jax.ShapeDtypeStruct((rows, HEAD_COLS), BF16)] * 2 + [jax.ShapeDtypeStruct((rows // 2, HEAD_COLS), BF16)] * 2,
        compiler_params=params(1),
        cost_estimate=pl.CostEstimate(flops=10_000_000, bytes_accessed=23_000_000, transcendentals=0),
    )(sc, w)


def fill_expert_weights(sc, wg_own, wu_own, gu1, rx2, ry2, rx3, ry3, wd_own, wd1, wgu, wd):
    core, rep = sc[0], sc[2]
    wgu[0:128, 0:896] = wg_own[0, 0].astype(BF16)
    wgu[0:128, 896:1792] = wu_own[0, 0].astype(BF16)
    wgu[128:256, 0:896] = gu1[0, 0]
    wgu[128:256, 896:1792] = gu1[1, 0]
    by_x = pl.ds(pl.multiple_of(rep * 896, 128), 896)
    by_y = pl.ds(pl.multiple_of((1 - rep) * 896, 128), 896)
    wgu[256:384, by_x] = rx2[0]
    wgu[384:512, by_x] = rx3[0]
    wgu[256:384, by_y] = ry2[0]
    wgu[384:512, by_y] = ry3[0]
    wd[pl.ds(pl.multiple_of(core * 448, 64), 448), :] = wd_own[0, 0].astype(BF16)
    wd[pl.ds(pl.multiple_of((1 - core) * 448, 64), 448), :] = wd1[0]


def expert_weight_specs(layer):
    own = lambda j, t, sc: (layer, 2 * j + sc[0], 0, sc[1])
    return [
        pl.BlockSpec((1, 1, 128, 896), own),
        pl.BlockSpec((1, 1, 128, 896), own),
        pl.BlockSpec((2, 1, 128, 896), lambda j, t, sc: (0, j, 0, 0)),
        pl.BlockSpec((1, 128, 896), lambda j, t, sc: (j, 0, 0)),
        pl.BlockSpec((1, 128, 896), lambda j, t, sc: (j, 0, 0)),
        pl.BlockSpec((1, 128, 896), lambda j, t, sc: (j, 0, 0)),
        pl.BlockSpec((1, 128, 896), lambda j, t, sc: (j, 0, 0)),
        pl.BlockSpec((1, 1, 448, 512), lambda j, t, sc: (layer, 2 * j + sc[0], 0, 0)),
        pl.BlockSpec((1, 448, 512), lambda j, t, sc: (j, 0, 0)),
    ]


EXPERT_SCRATCH = [pltpu.VMEM((512, 1792), BF16), pltpu.VMEM((896, 512), BF16)]


def expert_column(comb, expert):
    lanes = lax.broadcasted_iota(jnp.int32, comb.shape, 1)
    return jnp.sum(jnp.where(lanes == expert, comb, 0.0), axis=1, keepdims=True)


def expert_forward_kernel(sc, b_ref, comb_ref, wg_own, wu_own, gu1, rx2, ry2, rx3, ry3, wd_own, wd1, out_ref, wgu, wd):
    j, t = pl.program_id(0), pl.program_id(1)
    tile = b_ref.shape[0]

    @pl.when(t == 0)
    def _():
        fill_expert_weights(sc, wg_own, wu_own, gu1, rx2, ry2, rx3, ry3, wd_own, wd1, wgu, wd)

    b = permuted_columns(b_ref, sc[3])
    both = dot_nn(b, wgu[...])
    gate, up = both[:, 0:896], both[:, 896:1792]
    hidden = (gate * jax.nn.sigmoid(gate) * up).astype(BF16)
    weighted = dot_nn(hidden, wd[...]) * expert_column(comb_ref[...], 2 * j + sc[0])
    rows = pl.ds(pl.multiple_of(t * tile, tile), tile)

    @pl.when(j == 0)
    def _():
        out_ref[rows, :] = weighted

    @pl.when(j != 0)
    def _():
        out_ref[rows, :] += weighted


def expert_forward(sc, layer, b_rows, comb, w_gate, w_up, pieces, w_down, wd1):
    rows, width = b_rows.shape
    tile = 1024
    return pl.pallas_call(
        expert_forward_kernel,
        grid_spec=pltpu.PrefetchScalarGridSpec(
            num_scalar_prefetch=1,
            grid=(4, rows // tile),
            in_specs=[
                pl.BlockSpec((tile, width), lambda j, t, sc: (t, 0)),
                pl.BlockSpec((tile, 8), lambda j, t, sc: (t, 0)),
            ] + expert_weight_specs(layer),
            out_specs=pl.BlockSpec((rows, width), lambda j, t, sc: (0, 0)),
            scratch_shapes=EXPERT_SCRATCH,
        ),
        out_shape=jax.ShapeDtypeStruct((rows, width), F32),
        compiler_params=params(2),
        cost_estimate=pl.CostEstimate(flops=11_300_000_000, bytes_accessed=20_000_000, transcendentals=3_700_000),
    )(sc, b_rows, comb, w_gate, w_up, *pieces, w_down, wd1)


SLOT_TILE = 256


def slot_gradients(b_sel, d_sel, weight, wgu, wd):
    both = dot_nn(b_sel, wgu[...])
    gate, up = both[:, 0:896], both[:, 896:1792]
    sig = jax.nn.sigmoid(gate)
    silu = gate * sig
    hidden = (silu * up).astype(BF16).astype(F32)
    d_hidden = dot_nt(d_sel, wd[...])
    d_weight = jnp.sum(hidden * d_hidden, axis=1, keepdims=True)
    d_hidden = (d_hidden * weight).astype(BF16).astype(F32)
    d_up = (d_hidden * silu).astype(BF16)
    d_gate = (d_hidden * up * (sig * (1.0 + gate * (1.0 - sig)))).astype(BF16)
    return (hidden * weight).astype(BF16), jnp.concatenate([d_gate, d_up], axis=1), d_weight


def load_tokens(rows_ref, b_ref, d_ref, me):
    rows_ref[:, 0:512] = permuted_columns(b_ref, me)
    rows_ref[:, 512:1024] = d_ref[...].astype(BF16)


def select_slots(rank_row, comb_row, m, tokens_ref):
    index = lax.broadcasted_iota(jnp.int32, (SLOT_TILE, rank_row.shape[1]), 0) + m * SLOT_TILE
    chosen = index == rank_row
    picked = dot_nn(jnp.where(chosen, 1.0, 0.0).astype(BF16), tokens_ref[...])
    weight = jnp.sum(jnp.where(chosen, comb_row, 0.0), axis=1, keepdims=True)
    return chosen, picked[:, 0:512], picked[:, 512:1024], weight


def slot_tiles(sc, group, expert):
    return (sc[4 + group * 8 + expert] + (SLOT_TILE - 1)) // SLOT_TILE


def expert_dgrad_kernel(sc, b_ref, d_ref, rank_ref, rank_col_ref, comb_ref, wg_own, wu_own, gu1, rx2, ry2, rx3, ry3, wd_own, wd1,
                        db_ref, wgu, wd, tokens_ref, db_acc, dw_acc):
    j = pl.program_id(0)
    core, rep, me = sc[0], sc[2], sc[3]
    expert = 2 * j + core

    @pl.when(j == 0)
    def _():
        load_tokens(tokens_ref, b_ref, d_ref, me)
        db_acc[...] = jnp.zeros_like(db_acc)
        dw_acc[...] = jnp.zeros_like(dw_acc)

    fill_expert_weights(sc, wg_own, wu_own, gu1, rx2, ry2, rx3, ry3, wd_own, wd1, wgu, wd)

    row = pl.ds(expert, 1)

    def slots(m, carry):
        chosen, b_sel, d_sel, weight = select_slots(rank_ref[0, row, :], comb_ref[row, :], m, tokens_ref)
        _, d_both, d_weight = slot_gradients(b_sel.astype(BF16), d_sel.astype(BF16), weight, wgu, wd)
        db = dot_nt(d_both, wgu[...])
        high = db.astype(BF16)
        rest = db - high.astype(F32)
        middle = rest.astype(BF16)
        low = (rest - middle.astype(F32)).astype(BF16)
        rank_all = rank_col_ref[0]
        lanes = lax.broadcasted_iota(jnp.int32, rank_all.shape, 1)
        rank_col = jnp.sum(jnp.where(lanes == expert, rank_all, 0), axis=1, keepdims=True)
        index = lax.broadcasted_iota(jnp.int32, (rank_all.shape[0], SLOT_TILE), 1) + m * SLOT_TILE
        spread = jnp.where(index == rank_col, 1.0, 0.0).astype(BF16)
        db_acc[...] += dot_nn(jnp.concatenate([spread] * 3, axis=1), jnp.concatenate([high, middle, low], axis=0))
        dw_acc[row, :] += jnp.sum(jnp.where(chosen, d_weight, 0.0), axis=0, keepdims=True)
        return carry

    lax.fori_loop(0, slot_tiles(sc, rep, expert), slots, 0)

    @pl.when(j == pl.num_programs(0) - 1)
    def _():
        for k in range(4):
            db_ref[:, pl.ds(pl.multiple_of((me ^ k) * 128, 128), 128)] = db_acc[:, k * 128:(k + 1) * 128]
        db_ref[:, 512:640] = dw_acc[...].T


def expert_dgrad(sc, layer, b_group, d_all, ranks, rank_cols, comb, w_gate, w_up, pieces, w_down, wd1):
    rows, width = b_group.shape
    return pl.pallas_call(
        expert_dgrad_kernel,
        grid_spec=pltpu.PrefetchScalarGridSpec(
            num_scalar_prefetch=1,
            grid=(4, 1),
            in_specs=[
                pl.BlockSpec((rows, width), lambda j, t, sc: (0, 0)),
                pl.BlockSpec((rows, width), lambda j, t, sc: (sc[2], 0)),
                pl.BlockSpec((1, 8, rows), lambda j, t, sc: (sc[2], 0, 0)),
                pl.BlockSpec((1, rows, 8), lambda j, t, sc: (sc[2], 0, 0)),
                pl.BlockSpec((8, rows), lambda j, t, sc: (0, 0)),
            ] + expert_weight_specs(layer),
            out_specs=pl.BlockSpec((rows, 640), lambda j, t, sc: (0, 0)),
            scratch_shapes=EXPERT_SCRATCH + [pltpu.VMEM((rows, 2 * width), BF16), pltpu.VMEM((rows, width), F32), pltpu.VMEM((128, rows), F32)],
        ),
        out_shape=jax.ShapeDtypeStruct((rows, 640), F32),
        compiler_params=params(2),
        cost_estimate=pl.CostEstimate(flops=15_000_000_000, bytes_accessed=25_000_000, transcendentals=2_000_000),
    )(sc, b_group, d_all, ranks, rank_cols, comb, w_gate, w_up, *pieces, w_down, wd1)


def expert_wgrad_kernel(sc, b_own, b_other, d_own, d_other, rank_ref, comb_own, comb_other,
                        wg_own, wu_own, gu1, rx2, ry2, rx3, ry3, wd_own, wd1,
                        own_ref, near_ref, far2_ref, far3_ref, down_own_ref, down_other_ref, wgu, wd, tokens_ref, comb_ref, down_acc):
    j, group = pl.program_id(0), pl.program_id(1)
    core, rep, me = sc[0], sc[2], sc[3]
    expert = 2 * j + core

    @pl.when((j == 0) & (group == 0))
    def _():
        load_tokens(tokens_ref.at[rep], b_own, d_own, me)
        load_tokens(tokens_ref.at[1 - rep], b_other, d_other, me)
        comb_ref[rep] = comb_own[...]
        comb_ref[1 - rep] = comb_other[...]

    @pl.when(group == 0)
    def _():
        fill_expert_weights(sc, wg_own, wu_own, gu1, rx2, ry2, rx3, ry3, wd_own, wd1, wgu, wd)
        for ref in (own_ref, near_ref, far2_ref, far3_ref, down_acc):
            ref[...] = jnp.zeros_like(ref)

    row = pl.ds(expert, 1)

    def slots(m, carry):
        _, b_sel, d_sel, weight = select_slots(rank_ref[0, row, :], comb_ref[group, row, :], m, tokens_ref.at[group])
        hidden, d_both, _ = slot_gradients(b_sel.astype(BF16), d_sel.astype(BF16), weight, wgu, wd)
        bt = b_sel.T.astype(BF16)
        dt = d_sel.T.astype(BF16)
        dw = dot_nn(bt[0:256], d_both)
        for matrix in range(2):
            cols = slice(matrix * 896, matrix * 896 + 896)
            own_ref[matrix, 0] += dw[0:128, cols]
            near_ref[matrix, 0] += dw[128:256, cols]
        dw = dot_nn(bt[256:512], jnp.where(rep == 0, d_both[:, 0:896], d_both[:, 896:1792]))
        far2_ref[0] += dw[0:128]
        far3_ref[0] += dw[128:256]
        down_acc[...] += dot_nn(dt, hidden)
        return carry

    lax.fori_loop(0, slot_tiles(sc, group, expert), slots, 0)

    @pl.when(group == 1)
    def _():
        down_t = down_acc[...].T
        lower, upper = down_t[0:448], down_t[448:896]

        @pl.when(core == 0)
        def _():
            down_own_ref[0] = lower
            down_other_ref[0] = upper

        @pl.when(core != 0)
        def _():
            down_own_ref[0] = upper
            down_other_ref[0] = lower


def expert_wgrad(sc, layer, b_own, b_other, d_all, ranks, comb_own, comb_other, w_gate, w_up, pieces, w_down, wd1):
    rows, width = b_own.shape
    once = pl.BlockSpec((rows, width), lambda j, g, t, sc: (0, 0))
    weights = [pl.BlockSpec(spec.block_shape, functools.partial(lambda index, j, g, t, sc: index(j, t, sc), spec.index_map)) for spec in expert_weight_specs(layer)]
    return pl.pallas_call(
        expert_wgrad_kernel,
        grid_spec=pltpu.PrefetchScalarGridSpec(
            num_scalar_prefetch=1,
            grid=(4, 2, 1),
            in_specs=[once] * 2 + [
                pl.BlockSpec((rows, width), lambda j, g, t, sc: (sc[2], 0)),
                pl.BlockSpec((rows, width), lambda j, g, t, sc: (1 - sc[2], 0)),
                pl.BlockSpec((1, 8, rows), lambda j, g, t, sc: (g, 0, 0)),
                pl.BlockSpec((8, rows), lambda j, g, t, sc: (0, 0)),
                pl.BlockSpec((8, rows), lambda j, g, t, sc: (0, 0)),
            ] + weights,
            out_specs=[
                pl.BlockSpec((2, 1, 128, 896), lambda j, g, t, sc: (0, j, 0, 0)),
                pl.BlockSpec((2, 1, 128, 896), lambda j, g, t, sc: (0, j, 0, 0)),
                pl.BlockSpec((1, 128, 896), lambda j, g, t, sc: (j, 0, 0)),
                pl.BlockSpec((1, 128, 896), lambda j, g, t, sc: (j, 0, 0)),
                pl.BlockSpec((1, 448, 512), lambda j, g, t, sc: (j, 0, 0)),
                pl.BlockSpec((1, 448, 512), lambda j, g, t, sc: (j, 0, 0)),
            ],
            scratch_shapes=EXPERT_SCRATCH + [pltpu.VMEM((2, rows, 2 * width), BF16), pltpu.VMEM((2, 8, rows), F32), pltpu.VMEM((512, 896), F32)],
        ),
        out_shape=[
            jax.ShapeDtypeStruct((2, 4, 128, 896), F32),
            jax.ShapeDtypeStruct((2, 4, 128, 896), F32),
            jax.ShapeDtypeStruct((4, 128, 896), F32),
            jax.ShapeDtypeStruct((4, 128, 896), F32),
            jax.ShapeDtypeStruct((4, 448, 512), F32),
            jax.ShapeDtypeStruct((4, 448, 512), F32),
        ],
        compiler_params=params(3),
        cost_estimate=pl.CostEstimate(flops=30_000_000_000, bytes_accessed=50_000_000, transcendentals=4_000_000),
    )(sc, b_own, b_other, d_all, d_all, ranks, comb_own, comb_other, w_gate, w_up, *pieces, w_down, wd1)


HEAD_COLS = 8192
HEAD_BLOCK = 1024
HEAD_TILE = 1024
HEAD_HALF = 16000
HEAD_SHIFT = 7808
HEAD_OVERLAP = HEAD_COLS - HEAD_SHIFT


def head_start(x, core):
    return x * HEAD_HALF + core * HEAD_SHIFT


def fill_head_weights(sc, own, p1, rx2, ry2, rx3, ry3, w):
    rep = sc[2]
    w[0:128, :] = own[...]
    w[128:256, :] = p1[...]
    for k, (rx, ry) in ((2, (rx2, ry2)), (3, (rx3, ry3))):
        w[pl.ds(pl.multiple_of(k * 128 + rep * 64, 64), 64), :] = rx[...]
        w[pl.ds(pl.multiple_of(k * 128 + (1 - rep) * 64, 64), 64), :] = ry[...]


def head_weight_specs():
    return [pl.BlockSpec((128, HEAD_BLOCK), lambda i, sc: (0, i))] * 2 + [pl.BlockSpec((64, HEAD_BLOCK), lambda i, sc: (0, i))] * 4


def head_stats_kernel(sc, x_ref, own, p1, rx2, ry2, rx3, ry3, out_ref, w, xp, m_acc, s_acc):
    i = pl.program_id(0)
    rows = x_ref.shape[0]

    @pl.when(i == 0)
    def _():
        xp[...] = permuted_columns(x_ref, sc[3])
        m_acc[...] = jnp.full((rows, 128), -1e30, F32)
        s_acc[...] = jnp.zeros((rows, 128), F32)

    fill_head_weights(sc, own, p1, rx2, ry2, rx3, ry3, w)
    first_new = jnp.where((sc[0] == 1) & (i == 0), HEAD_OVERLAP, 0)
    tiles = [slice(t, t + HEAD_TILE) for t in range(0, rows, HEAD_TILE)]

    def update(tile, logits):
        pieces = []
        for q in range(HEAD_BLOCK // 128):
            piece = logits[:, q * 128:(q + 1) * 128]
            if q * 128 < HEAD_OVERLAP:
                piece = piece + jnp.where(q * 128 >= first_new, 0.0, -1e30)
            pieces.append(piece)
        peak = m_acc[tile, :]
        top = functools.reduce(jnp.maximum, pieces, peak)
        total = s_acc[tile, :] * jnp.exp(peak - top)
        for piece in pieces:
            total = total + jnp.exp(piece - top)
        m_acc[tile, :] = top
        s_acc[tile, :] = total

    ahead = dot_nn(xp[tiles[0], :], w[...])
    for n, tile in enumerate(tiles):
        logits = ahead
        if n + 1 < len(tiles):
            ahead = dot_nn(xp[tiles[n + 1], :], w[...])
        update(tile, logits)

    @pl.when(i == pl.num_programs(0) - 1)
    def _():
        top = m_acc[...]
        highest = jnp.max(top, axis=1, keepdims=True)
        out_ref[:, 0:1] = highest
        out_ref[:, 1:2] = jnp.sum(s_acc[...] * jnp.exp(top - highest), axis=1, keepdims=True)


def head_stats(sc, x_rows, pieces):
    rows, width = x_rows.shape
    return pl.pallas_call(
        head_stats_kernel,
        grid_spec=pltpu.PrefetchScalarGridSpec(
            num_scalar_prefetch=1,
            grid=(HEAD_COLS // HEAD_BLOCK,),
            in_specs=[pl.BlockSpec((rows, width), lambda i, sc: (0, 0))] + head_weight_specs(),
            out_specs=pl.BlockSpec((rows, 8), lambda i, sc: (0, 0)),
            scratch_shapes=[pltpu.VMEM((width, HEAD_BLOCK), BF16), pltpu.VMEM((rows, width), BF16)] + [pltpu.VMEM((rows, 128), F32)] * 2,
        ),
        out_shape=jax.ShapeDtypeStruct((rows, 8), F32),
        compiler_params=params(1),
        cost_estimate=pl.CostEstimate(flops=17_000_000_000, bytes_accessed=25_000_000, transcendentals=16_800_000),
    )(sc, x_rows, *pieces)


def head_dx_kernel(sc, x_ref, label_ref, lse_ref, own, p1, rx2, ry2, rx3, ry3, dl_ref, dx_ref, picked_ref, w, xp, dx_acc, picked_acc):
    i = pl.program_id(0)
    core, x, rep, me = sc[0], sc[1], sc[2], sc[3]
    rows = x_ref.shape[0]
    half = rows // 2

    @pl.when(i == 0)
    def _():
        xp[...] = permuted_columns(x_ref, me)
        dx_acc[...] = jnp.zeros_like(dx_acc)
        picked_acc[...] = jnp.zeros_like(picked_acc)

    fill_head_weights(sc, own, p1, rx2, ry2, rx3, ry3, w)
    start = head_start(x, core) + i * HEAD_BLOCK
    first_new = jnp.where((core == 1) & (i == 0), HEAD_OVERLAP, 0)
    cols = lax.broadcasted_iota(jnp.int32, (HEAD_TILE, HEAD_BLOCK), 1)
    count = half // HEAD_TILE
    tiles = []
    for side in (rep, 1 - rep):
        for t in range(count):
            tiles.append(pl.ds(pl.multiple_of(side * half + t * HEAD_TILE, HEAD_TILE), HEAD_TILE))

    def gradient(tile, logits):
        hit = cols == label_ref[tile, :] - start
        prob = jnp.exp(logits - lse_ref[tile, :])
        picked = jnp.where(hit, logits, 0.0)
        picked_acc[...] += sum(jnp.where(q * 128 >= first_new, 1.0, 0.0) * jnp.sum(picked[:, q * 128:(q + 1) * 128].reshape(HEAD_TILE // 8, 8, 128), axis=0)
                               for q in range(HEAD_BLOCK // 128))
        d_logits = (jnp.where(hit, prob - 1.0, prob) * (1.0 / rows)).astype(BF16)
        dl_ref[tile, :] = d_logits
        return d_logits

    def project(n, d_logits):
        overlap = d_logits[:, 0:HEAD_OVERLAP]
        overlap = jnp.where(first_new == 0, overlap.astype(F32), 0.0).astype(BF16)
        masked = jnp.concatenate([overlap, d_logits[:, HEAD_OVERLAP:]], axis=1)
        dx_acc[n * HEAD_TILE:(n + 1) * HEAD_TILE, :] += dot_nt(masked, w[...])

    ahead = dot_nn(xp[tiles[0], :], w[...])
    for n, tile in enumerate(tiles):
        logits = ahead
        if n + 1 < len(tiles):
            ahead = dot_nn(xp[tiles[n + 1], :], w[...])
        d_logits = gradient(tile, logits)
        if n < count:
            project(n, d_logits)

    @pl.when(i == pl.num_programs(0) - 1)
    def _():
        for k in range(4):
            dx_ref[:, pl.ds(pl.multiple_of((me ^ k) * 128, 128), 128)] = dx_acc[:, k * 128:(k + 1) * 128]
        picked_ref[...] = picked_acc[...]


def head_dx(sc, x_rows, labels, lse, pieces):
    rows, width = x_rows.shape
    return pl.pallas_call(
        head_dx_kernel,
        grid_spec=pltpu.PrefetchScalarGridSpec(
            num_scalar_prefetch=1,
            grid=(HEAD_COLS // HEAD_BLOCK,),
            in_specs=[
                pl.BlockSpec((rows, width), lambda i, sc: (0, 0)),
                pl.BlockSpec((rows, 1), lambda i, sc: (0, 0)),
                pl.BlockSpec((rows, 1), lambda i, sc: (0, 0)),
            ] + head_weight_specs(),
            out_specs=[pl.BlockSpec((rows, HEAD_BLOCK), lambda i, sc: (0, i)), pl.BlockSpec((rows // 2, width), lambda i, sc: (0, 0)),
                       pl.BlockSpec((8, 128), lambda i, sc: (0, 0))],
            scratch_shapes=[pltpu.VMEM((width, HEAD_BLOCK), BF16), pltpu.VMEM((rows, width), BF16), pltpu.VMEM((rows // 2, width), F32),
                            pltpu.VMEM((8, 128), F32)],
        ),
        out_shape=[jax.ShapeDtypeStruct((rows, HEAD_COLS), BF16), jax.ShapeDtypeStruct((rows // 2, width), F32), jax.ShapeDtypeStruct((8, 128), F32)],
        compiler_params=params(1),
        cost_estimate=pl.CostEstimate(flops=26_000_000_000, bytes_accessed=60_000_000, transcendentals=16_800_000),
    )(sc, x_rows, labels, lse, *pieces)


def head_dw_kernel(sc, xt_ref, dl_ref, d0, d1, d2, d3, xt):
    @pl.when(pl.program_id(0) == 0)
    def _():
        me, rep = sc[3], sc[2]
        for k in range(2):
            xt[k * 128:(k + 1) * 128, :] = xt_ref[pl.ds(pl.multiple_of((me ^ k) * 128, 128), 128), :]
        for k in range(2, 4):
            xt[128 + k * 64:192 + k * 64, :] = xt_ref[pl.ds(pl.multiple_of((me ^ k) * 128 + rep * 64, 64), 64), :]

    dw = dot_nn(xt[...], dl_ref[...])
    d0[...] = dw[0:128]
    d1[...] = dw[128:256]
    d2[...] = dw[256:320]
    d3[...] = dw[320:384]


def head_dw(sc, x_cols, dl):
    width, rows = x_cols.shape
    block = 512
    return pl.pallas_call(
        head_dw_kernel,
        grid_spec=pltpu.PrefetchScalarGridSpec(
            num_scalar_prefetch=1,
            grid=(HEAD_COLS // block,),
            in_specs=[
                pl.BlockSpec((width, rows), lambda i, sc: (0, 0)),
                pl.BlockSpec((rows, block), lambda i, sc: (0, i)),
            ],
            out_specs=[pl.BlockSpec((128, block), lambda i, sc: (0, i))] * 2 + [pl.BlockSpec((64, block), lambda i, sc: (0, i))] * 2,
            scratch_shapes=[pltpu.VMEM((384, rows), BF16)],
        ),
        out_shape=[jax.ShapeDtypeStruct((128, HEAD_COLS), F32)] * 2 + [jax.ShapeDtypeStruct((64, HEAD_COLS), F32)] * 2,
        compiler_params=params(1),
        cost_estimate=pl.CostEstimate(flops=13_000_000_000, bytes_accessed=52_000_000, transcendentals=0),
    )(sc, x_cols, dl)


def update_gate_up_kernel(matrix, sc, rate, w_ref, own, p1, rx2, ry2, rx3, ry3, *rest):
    out_ref = rest[-1]
    s = pl.program_id(0)
    x, rep = sc[1], sc[2]
    lr = rate[0]
    near = pl.ds(pl.multiple_of(x * 896, 128), 896)
    far = pl.ds(pl.multiple_of((1 - x) * 896, 128), 896)

    def put(cols, grad):
        out_ref[0, 0, :, cols] = w_ref[0, 0, :, cols] - lr * grad

    @pl.when(s == 0)
    def _():
        put(near, own[0, 0])
        put(far, jnp.where(rep == matrix, rx2[0], ry2[0]))

    @pl.when(s == 1)
    def _():
        put(near, p1[0, 0])
        put(far, jnp.where(rep == matrix, rx3[0], ry3[0]))


def update_gate_up(sc, rate, layer, matrix, w, dgu, p1, rx2, ry2, rx3, ry3, previous=None):
    whole = lambda s, j, sc: (layer, 2 * j + jnp.where(s == 0, sc[0], 1 - sc[0]), 0, 0)
    early = lambda s, j: jnp.where(s == 0, j, 3)
    late = lambda s, j: jnp.where(s == 0, 0, j)
    in_specs = [
        pl.BlockSpec(memory_space=pltpu.SMEM),
        pl.BlockSpec((1, 1, 128, 1792), whole),
        pl.BlockSpec((1, 1, 128, 896), lambda s, j, sc: (matrix, early(s, j), 0, 0)),
        pl.BlockSpec((1, 1, 128, 896), lambda s, j, sc: (matrix, late(s, j), 0, 0)),
        pl.BlockSpec((1, 128, 896), lambda s, j, sc: (early(s, j), 0, 0)),
        pl.BlockSpec((1, 128, 896), lambda s, j, sc: (early(s, j), 0, 0)),
        pl.BlockSpec((1, 128, 896), lambda s, j, sc: (late(s, j), 0, 0)),
        pl.BlockSpec((1, 128, 896), lambda s, j, sc: (late(s, j), 0, 0)),
    ]
    args = [sc, rate, w, dgu, p1, rx2, ry2, rx3, ry3]
    aliases = {}
    if previous is not None:
        in_specs.append(pl.BlockSpec(memory_space=pl.ANY))
        aliases = {len(args): 0}
        args.append(previous)
    return pl.pallas_call(
        functools.partial(update_gate_up_kernel, matrix),
        grid_spec=pltpu.PrefetchScalarGridSpec(
            num_scalar_prefetch=1, grid=(2, 4), in_specs=in_specs, out_specs=pl.BlockSpec((1, 1, 128, 1792), whole),
        ),
        out_shape=jax.ShapeDtypeStruct(w.shape, F32),
        input_output_aliases=aliases,
        compiler_params=params(2),
        cost_estimate=pl.CostEstimate(flops=4_000_000, bytes_accessed=22_000_000, transcendentals=0),
        name="update_gate_up",
    )(*args)


def update_down_kernel(sc, rate, w_ref, own, p1, *rest):
    out_ref = rest[-1]
    s = pl.program_id(0)

    @pl.when(s == 0)
    def _():
        out_ref[0, 0] = w_ref[0, 0] - rate[0] * own[0]

    @pl.when(s == 1)
    def _():
        out_ref[0, 0] = w_ref[0, 0] - rate[0] * p1[0]


def update_down(sc, rate, layer, w, own, p1, previous=None):
    whole = lambda s, j, sc: (layer, 2 * j + jnp.where(s == 0, sc[0], 1 - sc[0]), 0, 0)
    in_specs = [
        pl.BlockSpec(memory_space=pltpu.SMEM),
        pl.BlockSpec((1, 1, 448, 512), whole),
        pl.BlockSpec((1, 448, 512), lambda s, j, sc: (jnp.where(s == 0, j, 3), 0, 0)),
        pl.BlockSpec((1, 448, 512), lambda s, j, sc: (jnp.where(s == 0, 0, j), 0, 0)),
    ]
    args = [sc, rate, w, own, p1]
    aliases = {}
    if previous is not None:
        in_specs.append(pl.BlockSpec(memory_space=pl.ANY))
        aliases = {len(args): 0}
        args.append(previous)
    return pl.pallas_call(
        update_down_kernel,
        grid_spec=pltpu.PrefetchScalarGridSpec(
            num_scalar_prefetch=1, grid=(2, 4), in_specs=in_specs, out_specs=pl.BlockSpec((1, 1, 448, 512), whole),
        ),
        out_shape=jax.ShapeDtypeStruct(w.shape, F32),
        input_output_aliases=aliases,
        compiler_params=params(2),
        cost_estimate=pl.CostEstimate(flops=4_000_000, bytes_accessed=22_000_000, transcendentals=0),
    )(*args)


def update_head_kernel(sc, rate, w_ref, own, p1, rx2, ry2, rx3, ry3, out_ref):
    half = pl.program_id(0) // (pl.num_programs(0) // 2)
    core, x, rep = sc[0], sc[1], sc[2]
    lr = rate[0]
    blocks = (
        (x, core, own[...]),
        (x, 1 - core, p1[...]),
        (1 - x, core, jnp.where(half == rep, rx2[...], ry2[...])),
        (1 - x, 1 - core, jnp.where(half == rep, rx3[...], ry3[...])),
    )
    for bx, bc, grad in blocks:
        cols = pl.ds(pl.multiple_of(head_start(bx, bc), 128), HEAD_COLS)
        out_ref[:, cols] = w_ref[:, cols] - lr * grad


def update_head(sc, rate, w, own, p1, rx2, ry2, rx3, ry3):
    rows, vocab = w.shape
    step = 16
    count = rows // step
    inner = count // 2
    return pl.pallas_call(
        update_head_kernel,
        grid_spec=pltpu.PrefetchScalarGridSpec(
            num_scalar_prefetch=1,
            grid=(count,),
            in_specs=[
                pl.BlockSpec(memory_space=pltpu.SMEM),
                pl.BlockSpec((step, vocab), lambda i, sc: (i, 0)),
                pl.BlockSpec((step, HEAD_COLS), lambda i, sc: (i, 0)),
                pl.BlockSpec((step, HEAD_COLS), lambda i, sc: (i, 0)),
            ] + [pl.BlockSpec((step, HEAD_COLS), lambda i, sc: (i % inner, 0))] * 4,
            out_specs=pl.BlockSpec((step, vocab), lambda i, sc: (i, 0)),
        ),
        out_shape=jax.ShapeDtypeStruct(w.shape, F32),
        compiler_params=params(1),
        cost_estimate=pl.CostEstimate(flops=8_000_000, bytes_accessed=50_000_000, transcendentals=0),
    )(sc, rate, w, own, p1, rx2, ry2, rx3, ry3)


def update_embedding_kernel(sc, rate, ids_ref, d_ref, w_ref, out_ref):
    rows = w_ref.shape[0]
    first = sc[3] * (pl.num_programs(0) * rows) + pl.program_id(0) * rows
    index = lax.broadcasted_iota(jnp.int32, (rows, ids_ref.shape[1]), 0) + first
    onehot = jnp.where(index == ids_ref[...], 1.0, 0.0).astype(BF16)
    out_ref[...] = w_ref[...] - rate[0] * dot_nn(onehot, d_ref[...])


def update_embedding(sc, rate, ids, d_rows, w):
    rows, width = w.shape
    step = 400
    tokens = d_rows.shape[0]
    return pl.pallas_call(
        update_embedding_kernel,
        grid_spec=pltpu.PrefetchScalarGridSpec(
            num_scalar_prefetch=1,
            grid=(rows // step,),
            in_specs=[
                pl.BlockSpec(memory_space=pltpu.SMEM),
                pl.BlockSpec((1, tokens), lambda i, sc: (0, 0)),
                pl.BlockSpec((tokens, width), lambda i, sc: (0, 0)),
                pl.BlockSpec((step, width), lambda i, sc: (i, 0)),
            ],
            out_specs=pl.BlockSpec((step, width), lambda i, sc: (i, 0)),
        ),
        out_shape=jax.ShapeDtypeStruct(w.shape, F32),
        compiler_params=params(1),
        cost_estimate=pl.CostEstimate(flops=17_000_000_000, bytes_accessed=35_000_000, transcendentals=0),
    )(sc, rate, ids, d_rows, w)


def peer_of(rep, me, other_rep, k):
    across = (me, me + 1 - 2 * (me % 2), (me + 2) % 4, 3 - me)[k]
    return (1 - rep if other_rep else rep), across


def exchange_kernel(both, in_ref, out_ref, send_sem, recv_sem):
    rep, me = lax.axis_index(REP), lax.axis_index(FSDP)
    slot = rep * 4 + me if both else me
    peers = [(other, k) for other in ((False, True) if both else (False,)) for k in range(4) if other or k]
    barrier = pltpu.get_barrier_semaphore()
    for other, k in peers:
        pl.semaphore_signal(barrier, inc=1, device_id=peer_of(rep, me, other, k), device_id_type=pl.DeviceIdType.MESH)
    pl.semaphore_wait(barrier, len(peers))
    copies = []
    for n, (other, k) in enumerate(peers):
        copy = pltpu.make_async_remote_copy(
            src_ref=in_ref, dst_ref=out_ref.at[slot], send_sem=send_sem.at[n], recv_sem=recv_sem.at[n],
            device_id=peer_of(rep, me, other, k), device_id_type=pl.DeviceIdType.MESH)
        copy.start()
        copies.append(copy)
    out_ref[slot] = in_ref[...]
    for copy in copies:
        copy.wait()


def exchange(value, both, collective_id):
    count = 8 if both else 4
    return pl.pallas_call(
        functools.partial(exchange_kernel, both),
        in_specs=[pl.BlockSpec(memory_space=pltpu.VMEM)],
        out_specs=pl.BlockSpec(memory_space=pltpu.VMEM),
        out_shape=jax.ShapeDtypeStruct((count,) + value.shape, value.dtype),
        scratch_shapes=[pltpu.SemaphoreType.DMA((count - 1,)), pltpu.SemaphoreType.DMA((count - 1,))],
        compiler_params=pltpu.CompilerParams(collective_id=collective_id, has_side_effects=True),
        cost_estimate=pl.CostEstimate(flops=1_000_000_000, bytes_accessed=100_000, transcendentals=0),
        name="exchange",
    )(value)


def row_major(value):
    return with_layout_constraint(value, Layout(major_to_minor=(0, 1)))


def to_peer(value, k):
    return lax.ppermute(value, FSDP, [(i, i ^ k) for i in range(4)])


def to_replica(value):
    return lax.ppermute(value, REP, [(0, 1), (1, 0)])


def solution(mesh):
    batch_spec = P((REP, FSDP))
    layer_spec = P(None, FSDP)
    expert_spec = P(None, None, FSDP)
    param_specs = (P(FSDP), layer_spec, layer_spec, layer_spec, layer_spec, layer_spec, layer_spec, layer_spec, expert_spec, expert_spec, expert_spec, P(FSDP), P(FSDP))
    in_specs = (batch_spec, batch_spec, batch_spec, P(None, (REP, FSDP)), P()) + param_specs
    out_specs = param_specs + (P(),)

    def train_step(tok_ids, tok_labels, tok_pos, expert_idx, learn_rate, embedding, w_query, w_key, w_value, w_attn_out, g_attn, g_mlp, w_router, w_gate, w_up, w_down, g_final, w_head):
        me = lax.axis_index(FSDP)
        rep = lax.axis_index(REP)
        core, x = me % 2, me // 2
        place = jnp.stack([core, x, rep, me]).astype(jnp.int32)
        rate = learn_rate.reshape(1)
        layers = w_query.shape[0]
        length = tok_ids.shape[1]
        tokens = 8 * length
        cos_tab, sin_tab = rope_tables(tok_pos[0])

        packed = jnp.concatenate([tok_ids, tok_labels, expert_idx[0, 0].T, expert_idx[1, 0].T, tok_ids, tok_labels], axis=0)
        packed = exchange(packed, True, 0)
        all_ids, all_labels = packed[:, 0].reshape(-1), packed[:, 1].reshape(-1, 1)
        group = tokens // 2
        chosen_all = [packed[:, 2 + 2 * layer:4 + 2 * layer].transpose(1, 0, 2).reshape(2, tokens) for layer in range(layers)]
        before = (lax.broadcasted_iota(jnp.int32, (group, group), 0) < lax.broadcasted_iota(jnp.int32, (group, group), 1)).astype(BF16)
        routes = []
        for layer in range(layers):
            experts = lax.broadcasted_iota(jnp.int32, (8, tokens), 0)
            mask = ((experts == chosen_all[layer][:1]) | (experts == chosen_all[layer][1:])).reshape(8, 2, group).transpose(1, 0, 2)
            rank = lax.dot_general(mask.astype(BF16), before, (((2,), (0,)), ((), ())), preferred_element_type=F32).astype(jnp.int32)
            rank = jnp.where(mask, rank, -1)
            counts = jnp.sum(mask.astype(jnp.int32), axis=2).reshape(-1)
            routes.append((jnp.concatenate([place, counts]), rank, rank.transpose(0, 2, 1)))
        sc = routes[0][0]

        def own_group(values, axis=0):
            return lax.dynamic_slice_in_dim(values, rep * group, group, axis)

        def relay(value, k):
            rx = to_peer(value, k)
            return rx, to_replica(rx)

        def near(value):
            return to_peer(value, 1)

        def send_experts(layer):
            gu1, mine2, mine3, wd1 = pack_experts(place, layer, w_gate, w_up, w_down)
            pieces = (near(gu1), *relay(mine2, 2), *relay(mine3, 3))
            return pieces, near(wd1)

        def send_head():
            own, p1, mine2, mine3 = pack_head(place, w_head)
            return [own, near(p1), *relay(mine2, 2), *relay(mine3, 3)]

        final_col = jnp.stack([g_final, jnp.zeros_like(g_final)])[:, :, None]
        small = jnp.concatenate([w_query, w_key, w_value, w_attn_out, w_router, g_attn[:, :, None], g_mlp[:, :, None], final_col], axis=2)
        whole = []
        for layer in range(layers):
            whole.append(lax.all_gather(small[layer].astype(BF16), FSDP, axis=0, tiled=True))
        cuts = (0, 512, 640, 768, 1280, 1288, 1289, 1290, 1291)

        def small_param(layer, slot):
            value = whole[layer][:, cuts[slot]:cuts[slot + 1]]
            return value[:, 0] if slot >= 5 else value

        local = own_group(all_ids) - me * embedding.shape[0]
        owned = (local >= 0) & (local < embedding.shape[0])
        rows = jnp.take(embedding, jnp.clip(local, 0, embedding.shape[0] - 1), axis=0)
        rows = jnp.where(owned[:, None], rows, 0.0).astype(BF16)
        residual = row_major(lax.psum_scatter(rows, FSDP, scatter_dimension=0, tiled=True).astype(F32))

        sent = [send_experts(layer) for layer in range(layers)]
        head_pieces = send_head()
        saved = []
        for layer in range(layers):
            w_q, w_k, w_v, w_o, w_r = (small_param(layer, slot) for slot in range(5))
            gain_a, gain_m = small_param(layer, 5), small_param(layer, 6)
            residual, attn_vjp = jax.vjp(functools.partial(attention_part, cos_tab=cos_tab, sin_tab=sin_tab), residual, w_q, w_k, w_v, w_o, gain_a)

            def routed(*values, layer=layer):
                return router_part(*values, chosen=expert_idx[layer, 0].T)

            (b, _), router_vjp = jax.vjp(routed, residual, gain_m, w_r)
            b_group = lax.all_gather(row_major(b), FSDP, axis=0, tiled=True)
            b_other = to_replica(b_group)
            other = lax.dynamic_slice_in_dim(chosen_all[layer], (1 - rep) * group, group, 1)
            comb = combine_weights(router_logits(b_group, w_r), own_group(chosen_all[layer], 1))
            comb_other = combine_weights(router_logits(b_other, w_r), other)
            pieces, wd1 = sent[layer]
            partial = expert_forward(sc, layer, b_group, comb.T, w_gate, w_up, pieces, w_down, wd1)
            residual = row_major(residual + lax.psum_scatter(partial, FSDP, scatter_dimension=0, tiled=True))
            saved.append((attn_vjp, router_vjp, b_group, b_other, comb, comb_other))

        final, final_vjp = jax.vjp(rms_norm, residual, small_param(0, 7))
        x_all = lax.all_gather(row_major(final), (REP, FSDP), axis=0, tiled=True)
        stats = head_stats(sc, x_all, head_pieces)
        stats = exchange(stats.T, False, 1)
        peak = jnp.max(stats[:, 0], axis=0)
        lse = peak + jnp.log(jnp.sum(stats[:, 1] * jnp.exp(stats[:, 0] - peak), axis=0))
        dl, dx, picked = head_dx(sc, x_all, all_labels, lse[:, None], head_pieces)
        dh0, dh1, dh2, dh3 = head_dw(sc, x_all.T, dl)
        d_final = row_major(lax.psum_scatter(dx, FSDP, scatter_dimension=0, tiled=True))
        d_residual, d_gain_final = final_vjp(d_final.astype(BF16))
        head_returns = [near(dh1), *relay(dh2, 2), *relay(dh3, 3)]
        new_head = update_head(sc, rate, w_head, dh0, *head_returns)

        small_grads = [None] * layers
        new_gate = new_up = new_down = None
        for layer in reversed(range(layers)):
            attn_vjp, router_vjp, b_group, b_other, comb, comb_other = saved[layer]
            d_all = lax.all_gather(row_major(d_residual), (REP, FSDP), axis=0, tiled=True)
            pieces, wd1 = sent[layer]
            scalars, ranks, rank_cols = routes[layer]
            db = expert_dgrad(scalars, layer, b_group, d_all, ranks, rank_cols, comb, w_gate, w_up, pieces, w_down, wd1)
            own, near1, far2, far3, down_own, down_other = expert_wgrad(scalars, layer, b_group, b_other, d_all, ranks, comb, comb_other, w_gate, w_up, pieces, w_down, wd1)
            returned = (*relay(far2, 2), *relay(far3, 3))
            gu1 = near(near1)
            down1 = near(down_other)
            new_gate = update_gate_up(sc, rate, layer, 0, w_gate, own, gu1, *returned, previous=new_gate)
            new_up = update_gate_up(sc, rate, layer, 1, w_up, own, gu1, *returned, previous=new_up)
            new_down = update_down(sc, rate, layer, w_down, down_own, down1, previous=new_down)
            db = row_major(lax.psum_scatter(db, FSDP, scatter_dimension=0, tiled=True))
            d_router_in, d_gain_m, d_wr = router_vjp((db[:, :512].astype(BF16), db[:, 512:520].T))
            d_residual = d_residual + d_router_in
            d_residual, d_wq, d_wk, d_wv, d_wo, d_gain_a = attn_vjp(d_residual)
            extra = d_gain_final if layer == 0 else jnp.full_like(d_gain_final, 0, F32) + jnp.sum(picked)
            grads = [d_wq, d_wk, d_wv, d_wo, d_wr, d_gain_a[:, None], d_gain_m[:, None], extra[:, None]]
            small_grads[layer] = jnp.concatenate([g.astype(F32) for g in grads], axis=1)

        d_rows = lax.all_gather(row_major(d_residual.astype(BF16)), (REP, FSDP), axis=0, tiled=True)
        new_embedding = update_embedding(sc, rate, all_ids[None, :], d_rows, embedding)

        small_grad = lax.psum_scatter(jnp.stack(small_grads), FSDP, scatter_dimension=1, tiled=True)
        small_grad = lax.psum(small_grad, REP)
        new_small = small - learn_rate * small_grad
        mean_loss = (jnp.sum(lse) - small_grad[1, 0, 1290] / 2) / tokens

        def new_param(slot):
            value = new_small[:, :, cuts[slot]:cuts[slot + 1]]
            return value[:, :, 0] if slot >= 5 else value

        return (new_embedding, new_param(0), new_param(1), new_param(2), new_param(3), new_param(5), new_param(6), new_param(4),
                new_gate, new_up, new_down, new_param(7)[0], new_head, mean_loss)


    return jax.shard_map(train_step, mesh=mesh, in_specs=in_specs, out_specs=out_specs, check_vma=False)
```

```python
import functools
import jax
import jax.numpy as jnp
from jax import lax
from jax.experimental import pallas as pl
from jax.experimental.pallas import tpu as pltpu
from jax.experimental.layout import Layout, with_layout_constraint
from jax.sharding import PartitionSpec as P

ZERO, ONE, TWO, ALL = 0, 1, 2, ...
LANES = 128
WIDTH = 512
FF_HALF = 896
HEAD_DIM = LANES
ROPE_THETA = 1000000.0
NORM_EPS = 1e-5
BF16 = jnp.bfloat16
F32 = jnp.float32
VMEM_LIMIT = 60 * 1024 * 1024
FSDP = 'fsdp'
REP = 'rep'


def rms_norm(residual, gain):
    mean_sq = jnp.mean(residual * residual, axis=-ONE, keepdims=True)
    return (residual * lax.rsqrt(mean_sq + NORM_EPS) * gain).astype(BF16)


def rope_tables(positions):
    inv_freq = ROPE_THETA ** (-jnp.arange(ZERO, HEAD_DIM, TWO, dtype=F32) / HEAD_DIM)
    angle = positions.astype(F32)[ALL, None] * inv_freq
    return jnp.cos(angle)[:, None, :], jnp.sin(angle)[:, None, :]


def apply_rope(heads, cos_tab, sin_tab):
    half_dim = heads.shape[-ONE] // TWO
    lower = heads[ALL, :half_dim]
    upper = heads[ALL, half_dim:]
    return jnp.concatenate([lower * cos_tab - upper * sin_tab, upper * cos_tab + lower * sin_tab], axis=-ONE)


def attention_part(residual, w_qkv, w_o, gain, cos_tab, sin_tab):
    length = residual.shape[ZERO]
    q_width = w_o.shape[ZERO]
    q_heads = q_width // HEAD_DIM
    normed = rms_norm(residual, gain)
    projected = jnp.dot(normed, w_qkv, preferred_element_type=F32)
    values = projected[:, q_width + HEAD_DIM:].astype(BF16)
    turned = apply_rope(projected[:, :q_width + HEAD_DIM].reshape(length, q_heads + ONE, HEAD_DIM), cos_tab, sin_tab).astype(BF16)
    query, keyed = turned[:, :q_heads], turned[:, q_heads]
    scores = jnp.einsum('qgd,sd->gqs', query, keyed, preferred_element_type=F32) * HEAD_DIM ** -0.5
    causal = lax.broadcasted_iota(jnp.int32, (length, length), ZERO) >= lax.broadcasted_iota(jnp.int32, (length, length), ONE)
    scores = jnp.where(causal, scores, -1e30)
    attn_probs = jax.nn.softmax(scores, axis=-ONE).astype(BF16)
    mixed = jnp.einsum('gqs,sd->qgd', attn_probs, values, preferred_element_type=F32).astype(BF16)
    mixed = mixed.reshape(length, q_width)
    return residual + jnp.dot(mixed, w_o, preferred_element_type=F32)


def combine_weights(logits, chosen):
    rows = lax.broadcasted_iota(jnp.int32, logits.shape, ZERO)
    first = rows == chosen[:ONE]
    second = rows == chosen[ONE:]
    r0 = jnp.sum(jnp.where(first, logits, 0.0), axis=ZERO, keepdims=True)
    r1 = jnp.sum(jnp.where(second, logits, 0.0), axis=ZERO, keepdims=True)
    gates = jax.nn.softmax(jnp.concatenate([r0, r1], axis=ZERO), axis=ZERO)
    return jnp.where(first, gates[:ONE], 0.0) + jnp.where(second, gates[ONE:], 0.0)


def router_logits(normed, w_r):
    return lax.dot_general(w_r, normed, (((ZERO,), (ONE,)), ((), ())), preferred_element_type=F32)


def router_part(residual, gain, w_r, chosen):
    normed = rms_norm(residual, gain)
    return normed, combine_weights(router_logits(normed, w_r), chosen)


def dot_nn(a, b):
    return jnp.dot(a, b, preferred_element_type=F32)


def dot_nt(a, b):
    return lax.dot_general(a, b, (((ONE,), (ONE,)), ((), ())), preferred_element_type=F32)


def params(steps):
    return pltpu.CompilerParams(dimension_semantics=("arbitrary",) * steps, vmem_limit_bytes=VMEM_LIMIT)


def permuted_columns(ref, me):
    return jnp.concatenate([ref[:, pl.ds(pl.multiple_of((me ^ k) * LANES, LANES), LANES)] for k in range(4)], axis=ONE)


def pack_experts_kernel(sc, gate1, up1, gate2, up2, gate3, up3, down1, out1, out2, out3, out_down):
    rep = sc[TWO]
    out1[ZERO, ZERO] = gate1[ZERO, ZERO].astype(BF16)
    out1[ONE, ZERO] = up1[ZERO, ZERO].astype(BF16)
    out2[ZERO] = jnp.where(rep == ZERO, gate2[ZERO, ZERO], up2[ZERO, ZERO]).astype(BF16)
    out3[ZERO] = jnp.where(rep == ZERO, gate3[ZERO, ZERO], up3[ZERO, ZERO]).astype(BF16)
    out_down[ZERO] = down1[ZERO, ZERO].astype(BF16)


def pack_experts(sc, layer, w_gate, w_up, w_down):
    def spec(own_core, own_half, matrix=None):
        def index(j, sc):
            step = j if matrix is None else jnp.where(sc[TWO] == matrix, j, ZERO)
            core = sc[ZERO] if own_core else ONE - sc[ZERO]
            return layer, TWO * step + core, ZERO, (sc[ONE] if own_half else ONE - sc[ONE])

        return pl.BlockSpec((ONE, ONE, LANES, FF_HALF), index)

    block = lambda j, sc: (j, ZERO, ZERO)
    return pl.pallas_call(
        pack_experts_kernel,
        grid_spec=pltpu.PrefetchScalarGridSpec(
            num_scalar_prefetch=ONE,
            grid=(4,),
            in_specs=[spec(False, True), spec(False, True), spec(True, False, ZERO), spec(True, False, ONE), spec(False, False, ZERO), spec(False, False, ONE),
                      pl.BlockSpec((ONE, ONE, 448, WIDTH), lambda j, sc: (layer, TWO * j + ONE - sc[ZERO], ZERO, ZERO))],
            out_specs=[pl.BlockSpec((TWO, ONE, LANES, FF_HALF), lambda j, sc: (ZERO, j, ZERO, ZERO)), pl.BlockSpec((ONE, LANES, FF_HALF), block), pl.BlockSpec((ONE, LANES, FF_HALF), block),
                       pl.BlockSpec((ONE, 448, WIDTH), block)],
        ),
        out_shape=[
            jax.ShapeDtypeStruct((TWO, 4, LANES, FF_HALF), BF16),
            jax.ShapeDtypeStruct((4, LANES, FF_HALF), BF16),
            jax.ShapeDtypeStruct((4, LANES, FF_HALF), BF16),
            jax.ShapeDtypeStruct((4, 448, WIDTH), BF16),
        ],
        compiler_params=params(ONE),
        cost_estimate=pl.CostEstimate(flops=10_000_000, bytes_accessed=17_000_000, transcendentals=ZERO),
    )(sc, w_gate, w_up, w_gate, w_up, w_gate, w_up, w_down)


def pack_head_kernel(sc, w_ref, out0, out1, out2, out3):
    core, x, rep = sc[ZERO], sc[ONE], sc[TWO]

    def part(xx, cc):
        return w_ref[:, pl.ds(pl.multiple_of(head_start(xx, cc), LANES), HEAD_COLS)].astype(BF16)

    out0[ALL] = part(x, core)
    out1[ALL] = part(x, ONE - core)

    @pl.when(pl.program_id(ZERO) // (pl.num_programs(ZERO) // TWO) == rep)
    def _():
        out2[ALL] = part(ONE - x, core)
        out3[ALL] = part(ONE - x, ONE - core)


def pack_head(sc, w):
    rows, vocab = w.shape
    step = 16
    count = rows // step
    half = lambda i, sc: (jnp.clip(i - sc[TWO] * (count // TWO), ZERO, count // TWO - ONE), ZERO)
    return pl.pallas_call(
        pack_head_kernel,
        grid_spec=pltpu.PrefetchScalarGridSpec(
            num_scalar_prefetch=ONE,
            grid=(count,),
            in_specs=[pl.BlockSpec((step, vocab), lambda i, sc: (i, ZERO))],
            out_specs=[pl.BlockSpec((step, HEAD_COLS), lambda i, sc: (i, ZERO))] * TWO + [pl.BlockSpec((step, HEAD_COLS), half)] * TWO,
        ),
        out_shape=[jax.ShapeDtypeStruct((rows, HEAD_COLS), BF16)] * TWO + [jax.ShapeDtypeStruct((rows // TWO, HEAD_COLS), BF16)] * TWO,
        compiler_params=params(ONE),
        cost_estimate=pl.CostEstimate(flops=10_000_000, bytes_accessed=23_000_000, transcendentals=ZERO),
    )(sc, w)


def fill_expert_weights(sc, wg_own, wu_own, gu1, rx2, ry2, rx3, ry3, wd_own, wd1, wgu, wd):
    core, rep = sc[ZERO], sc[TWO]
    wgu[ZERO:LANES, ZERO:FF_HALF] = wg_own[ZERO, ZERO].astype(BF16)
    wgu[ZERO:LANES, FF_HALF:1792] = wu_own[ZERO, ZERO].astype(BF16)
    wgu[LANES:256, ZERO:FF_HALF] = gu1[ZERO, ZERO]
    wgu[LANES:256, FF_HALF:1792] = gu1[ONE, ZERO]
    by_x = pl.ds(pl.multiple_of(rep * FF_HALF, LANES), FF_HALF)
    by_y = pl.ds(pl.multiple_of((ONE - rep) * FF_HALF, LANES), FF_HALF)
    wgu[256:384, by_x] = rx2[ZERO]
    wgu[384:WIDTH, by_x] = rx3[ZERO]
    wgu[256:384, by_y] = ry2[ZERO]
    wgu[384:WIDTH, by_y] = ry3[ZERO]
    wd[pl.ds(pl.multiple_of(core * 448, 64), 448), :] = wd_own[ZERO, ZERO].astype(BF16)
    wd[pl.ds(pl.multiple_of((ONE - core) * 448, 64), 448), :] = wd1[ZERO]


def expert_weight_specs(layer):
    own = lambda j, t, sc: (layer, TWO * j + sc[ZERO], ZERO, sc[ONE])
    return [
        pl.BlockSpec((ONE, ONE, LANES, FF_HALF), own),
        pl.BlockSpec((ONE, ONE, LANES, FF_HALF), own),
        pl.BlockSpec((TWO, ONE, LANES, FF_HALF), lambda j, t, sc: (ZERO, j, ZERO, ZERO)),
        pl.BlockSpec((ONE, LANES, FF_HALF), lambda j, t, sc: (j, ZERO, ZERO)),
        pl.BlockSpec((ONE, LANES, FF_HALF), lambda j, t, sc: (j, ZERO, ZERO)),
        pl.BlockSpec((ONE, LANES, FF_HALF), lambda j, t, sc: (j, ZERO, ZERO)),
        pl.BlockSpec((ONE, LANES, FF_HALF), lambda j, t, sc: (j, ZERO, ZERO)),
        pl.BlockSpec((ONE, ONE, 448, WIDTH), lambda j, t, sc: (layer, TWO * j + sc[ZERO], ZERO, ZERO)),
        pl.BlockSpec((ONE, 448, WIDTH), lambda j, t, sc: (j, ZERO, ZERO)),
    ]


EXPERT_SCRATCH = [pltpu.VMEM((WIDTH, 1792), BF16), pltpu.VMEM((FF_HALF, WIDTH), BF16)]


def expert_column(comb, expert):
    lanes = lax.broadcasted_iota(jnp.int32, comb.shape, ONE)
    return jnp.sum(jnp.where(lanes == expert, comb, 0.0), axis=ONE, keepdims=True)


def expert_forward_kernel(sc, b_ref, comb_ref, wg_own, wu_own, gu1, rx2, ry2, rx3, ry3, wd_own, wd1, out_ref, wgu, wd):
    j, t = pl.program_id(ZERO), pl.program_id(ONE)
    tile = b_ref.shape[ZERO]

    @pl.when(t == ZERO)
    def _():
        fill_expert_weights(sc, wg_own, wu_own, gu1, rx2, ry2, rx3, ry3, wd_own, wd1, wgu, wd)

    b = permuted_columns(b_ref, sc[3])
    both = dot_nn(b, wgu[ALL])
    gate, up = both[:, ZERO:FF_HALF], both[:, FF_HALF:1792]
    hidden = (gate * jax.nn.sigmoid(gate) * up).astype(BF16)
    weighted = dot_nn(hidden, wd[ALL]) * expert_column(comb_ref[ALL], TWO * j + sc[ZERO])
    rows = pl.ds(pl.multiple_of(t * tile, tile), tile)

    @pl.when(j == ZERO)
    def _():
        out_ref[rows, :] = weighted

    @pl.when(j != ZERO)
    def _():
        out_ref[rows, :] += weighted


def expert_forward(sc, layer, b_rows, comb, w_gate, w_up, pieces, w_down, wd1):
    rows, width = b_rows.shape
    tile = 1024
    return pl.pallas_call(
        expert_forward_kernel,
        grid_spec=pltpu.PrefetchScalarGridSpec(
            num_scalar_prefetch=ONE,
            grid=(4, rows // tile),
            in_specs=[
                pl.BlockSpec((tile, width), lambda j, t, sc: (t, ZERO)),
                pl.BlockSpec((tile, 8), lambda j, t, sc: (t, ZERO)),
            ] + expert_weight_specs(layer),
            out_specs=pl.BlockSpec((rows, width), lambda j, t, sc: (ZERO, ZERO)),
            scratch_shapes=EXPERT_SCRATCH,
        ),
        out_shape=jax.ShapeDtypeStruct((rows, width), F32),
        compiler_params=params(TWO),
        cost_estimate=pl.CostEstimate(flops=11_300_000_000, bytes_accessed=20_000_000, transcendentals=3_700_000),
    )(sc, b_rows, comb, w_gate, w_up, *pieces, w_down, wd1)


SLOT_TILE = 256


def slot_gradients(b_sel, d_sel, weight, wgu, wd):
    both = dot_nn(b_sel, wgu[ALL])
    gate, up = both[:, ZERO:FF_HALF], both[:, FF_HALF:1792]
    sig = jax.nn.sigmoid(gate)
    silu = gate * sig
    hidden = (silu * up).astype(BF16).astype(F32)
    d_hidden = dot_nt(d_sel, wd[ALL])
    d_weight = jnp.sum(hidden * d_hidden, axis=ONE, keepdims=True)
    d_hidden = (d_hidden * weight).astype(BF16).astype(F32)
    d_up = (d_hidden * silu).astype(BF16)
    d_gate = (d_hidden * up * (sig * (1.0 + gate * (1.0 - sig)))).astype(BF16)
    return (hidden * weight).astype(BF16), jnp.concatenate([d_gate, d_up], axis=ONE), d_weight


def load_tokens(rows_ref, b_ref, d_ref, me):
    rows_ref[:, ZERO:WIDTH] = permuted_columns(b_ref, me)
    rows_ref[:, WIDTH:1024] = d_ref[ALL].astype(BF16)


def select_slots(rank_row, comb_row, m, tokens_ref):
    index = lax.broadcasted_iota(jnp.int32, (SLOT_TILE, rank_row.shape[ONE]), ZERO) + m * SLOT_TILE
    chosen = index == rank_row
    picked = dot_nn(jnp.where(chosen, 1.0, 0.0).astype(BF16), tokens_ref[ALL])
    weight = jnp.sum(jnp.where(chosen, comb_row, 0.0), axis=ONE, keepdims=True)
    return chosen, picked[:, ZERO:WIDTH], picked[:, WIDTH:1024], weight


def slot_tiles(sc, group, expert):
    return (sc[4 + group * 8 + expert] + (SLOT_TILE - ONE)) // SLOT_TILE


def expert_dgrad_kernel(sc, b_ref, d_ref, rank_ref, rank_col_ref, comb_ref, wg_own, wu_own, gu1, rx2, ry2, rx3, ry3, wd_own, wd1,
                        db_ref, wgu, wd, tokens_ref, db_acc, dw_acc):
    j = pl.program_id(ZERO)
    core, rep, me = sc[ZERO], sc[TWO], sc[3]
    expert = TWO * j + core

    @pl.when(j == ZERO)
    def _():
        load_tokens(tokens_ref, b_ref, d_ref, me)
        db_acc[ALL] = jnp.zeros_like(db_acc)
        dw_acc[ALL] = jnp.zeros_like(dw_acc)

    fill_expert_weights(sc, wg_own, wu_own, gu1, rx2, ry2, rx3, ry3, wd_own, wd1, wgu, wd)

    row = pl.ds(expert, ONE)

    def slots(m, carry):
        chosen, b_sel, d_sel, weight = select_slots(rank_ref[ZERO, row, :], comb_ref[row, :], m, tokens_ref)
        _, d_both, d_weight = slot_gradients(b_sel.astype(BF16), d_sel.astype(BF16), weight, wgu, wd)
        db = dot_nt(d_both, wgu[ALL])
        high = db.astype(BF16)
        rest = db - high.astype(F32)
        middle = rest.astype(BF16)
        low = (rest - middle.astype(F32)).astype(BF16)
        rank_all = rank_col_ref[ZERO]
        lanes = lax.broadcasted_iota(jnp.int32, rank_all.shape, ONE)
        rank_col = jnp.sum(jnp.where(lanes == expert, rank_all, ZERO), axis=ONE, keepdims=True)
        index = lax.broadcasted_iota(jnp.int32, (rank_all.shape[ZERO], SLOT_TILE), ONE) + m * SLOT_TILE
        spread = jnp.where(index == rank_col, 1.0, 0.0).astype(BF16)
        db_acc[ALL] += dot_nn(jnp.concatenate([spread] * 3, axis=ONE), jnp.concatenate([high, middle, low], axis=ZERO))
        dw_acc[row, :] += jnp.sum(jnp.where(chosen, d_weight, 0.0), axis=ZERO, keepdims=True)
        return carry

    lax.fori_loop(ZERO, slot_tiles(sc, rep, expert), slots, ZERO)

    @pl.when(j == pl.num_programs(ZERO) - ONE)
    def _():
        for k in range(4):
            db_ref[:, pl.ds(pl.multiple_of((me ^ k) * LANES, LANES), LANES)] = db_acc[:, k * LANES:(k + ONE) * LANES]
        db_ref[:, WIDTH:640] = dw_acc[ALL].T


def expert_dgrad(sc, layer, b_group, d_all, ranks, rank_cols, comb, w_gate, w_up, pieces, w_down, wd1):
    rows, width = b_group.shape
    return pl.pallas_call(
        expert_dgrad_kernel,
        grid_spec=pltpu.PrefetchScalarGridSpec(
            num_scalar_prefetch=ONE,
            grid=(4, ONE),
            in_specs=[
                pl.BlockSpec((rows, width), lambda j, t, sc: (ZERO, ZERO)),
                pl.BlockSpec((rows, width), lambda j, t, sc: (sc[TWO], ZERO)),
                pl.BlockSpec((ONE, 8, rows), lambda j, t, sc: (sc[TWO], ZERO, ZERO)),
                pl.BlockSpec((ONE, rows, 8), lambda j, t, sc: (sc[TWO], ZERO, ZERO)),
                pl.BlockSpec((8, rows), lambda j, t, sc: (ZERO, ZERO)),
            ] + expert_weight_specs(layer),
            out_specs=pl.BlockSpec((rows, 640), lambda j, t, sc: (ZERO, ZERO)),
            scratch_shapes=EXPERT_SCRATCH + [pltpu.VMEM((rows, TWO * width), BF16), pltpu.VMEM((rows, width), F32), pltpu.VMEM((LANES, rows), F32)],
        ),
        out_shape=jax.ShapeDtypeStruct((rows, 640), F32),
        compiler_params=params(TWO),
        cost_estimate=pl.CostEstimate(flops=15_000_000_000, bytes_accessed=25_000_000, transcendentals=2_000_000),
    )(sc, b_group, d_all, ranks, rank_cols, comb, w_gate, w_up, *pieces, w_down, wd1)


def expert_wgrad_kernel(sc, b_own, b_other, d_own, d_other, rank_ref, comb_own, comb_other,
                        wg_own, wu_own, gu1, rx2, ry2, rx3, ry3, wd_own, wd1,
                        own_ref, near_ref, far2_ref, far3_ref, down_own_ref, down_other_ref, wgu, wd, tokens_ref, comb_ref, down_acc):
    j, group = pl.program_id(ZERO), pl.program_id(ONE)
    core, rep, me = sc[ZERO], sc[TWO], sc[3]
    expert = TWO * j + core

    @pl.when((j == ZERO) & (group == ZERO))
    def _():
        load_tokens(tokens_ref.at[rep], b_own, d_own, me)
        load_tokens(tokens_ref.at[ONE - rep], b_other, d_other, me)
        comb_ref[rep] = comb_own[ALL]
        comb_ref[ONE - rep] = comb_other[ALL]

    @pl.when(group == ZERO)
    def _():
        fill_expert_weights(sc, wg_own, wu_own, gu1, rx2, ry2, rx3, ry3, wd_own, wd1, wgu, wd)
        for ref in (own_ref, near_ref, far2_ref, far3_ref, down_acc):
            ref[ALL] = jnp.zeros_like(ref)

    row = pl.ds(expert, ONE)

    def slots(m, carry):
        _, b_sel, d_sel, weight = select_slots(rank_ref[ZERO, row, :], comb_ref[group, row, :], m, tokens_ref.at[group])
        hidden, d_both, _ = slot_gradients(b_sel.astype(BF16), d_sel.astype(BF16), weight, wgu, wd)
        bt = b_sel.T.astype(BF16)
        dt = d_sel.T.astype(BF16)
        dw = dot_nn(bt[ZERO:256], d_both)
        for matrix in range(TWO):
            cols = slice(matrix * FF_HALF, matrix * FF_HALF + FF_HALF)
            own_ref[matrix, ZERO] += dw[ZERO:LANES, cols]
            near_ref[matrix, ZERO] += dw[LANES:256, cols]
        dw = dot_nn(bt[256:WIDTH], jnp.where(rep == ZERO, d_both[:, ZERO:FF_HALF], d_both[:, FF_HALF:1792]))
        far2_ref[ZERO] += dw[ZERO:LANES]
        far3_ref[ZERO] += dw[LANES:256]
        down_acc[ALL] += dot_nn(dt, hidden)
        return carry

    lax.fori_loop(ZERO, slot_tiles(sc, group, expert), slots, ZERO)

    @pl.when(group == ONE)
    def _():
        down_t = down_acc[ALL].T
        lower, upper = down_t[ZERO:448], down_t[448:FF_HALF]

        @pl.when(core == ZERO)
        def _():
            down_own_ref[ZERO] = lower
            down_other_ref[ZERO] = upper

        @pl.when(core != ZERO)
        def _():
            down_own_ref[ZERO] = upper
            down_other_ref[ZERO] = lower


def expert_wgrad(sc, layer, b_own, b_other, d_all, ranks, comb_own, comb_other, w_gate, w_up, pieces, w_down, wd1):
    rows, width = b_own.shape
    once = pl.BlockSpec((rows, width), lambda j, g, t, sc: (ZERO, ZERO))
    weights = [pl.BlockSpec(spec.block_shape, functools.partial(lambda index, j, g, t, sc: index(j, t, sc), spec.index_map)) for spec in expert_weight_specs(layer)]
    return pl.pallas_call(
        expert_wgrad_kernel,
        grid_spec=pltpu.PrefetchScalarGridSpec(
            num_scalar_prefetch=ONE,
            grid=(4, TWO, ONE),
            in_specs=[once] * TWO + [
                pl.BlockSpec((rows, width), lambda j, g, t, sc: (sc[TWO], ZERO)),
                pl.BlockSpec((rows, width), lambda j, g, t, sc: (ONE - sc[TWO], ZERO)),
                pl.BlockSpec((ONE, 8, rows), lambda j, g, t, sc: (g, ZERO, ZERO)),
                pl.BlockSpec((8, rows), lambda j, g, t, sc: (ZERO, ZERO)),
                pl.BlockSpec((8, rows), lambda j, g, t, sc: (ZERO, ZERO)),
            ] + weights,
            out_specs=[
                pl.BlockSpec((TWO, ONE, LANES, FF_HALF), lambda j, g, t, sc: (ZERO, j, ZERO, ZERO)),
                pl.BlockSpec((TWO, ONE, LANES, FF_HALF), lambda j, g, t, sc: (ZERO, j, ZERO, ZERO)),
                pl.BlockSpec((ONE, LANES, FF_HALF), lambda j, g, t, sc: (j, ZERO, ZERO)),
                pl.BlockSpec((ONE, LANES, FF_HALF), lambda j, g, t, sc: (j, ZERO, ZERO)),
                pl.BlockSpec((ONE, 448, WIDTH), lambda j, g, t, sc: (j, ZERO, ZERO)),
                pl.BlockSpec((ONE, 448, WIDTH), lambda j, g, t, sc: (j, ZERO, ZERO)),
            ],
            scratch_shapes=EXPERT_SCRATCH + [pltpu.VMEM((TWO, rows, TWO * width), BF16), pltpu.VMEM((TWO, 8, rows), F32), pltpu.VMEM((WIDTH, FF_HALF), F32)],
        ),
        out_shape=[
            jax.ShapeDtypeStruct((TWO, 4, LANES, FF_HALF), F32),
            jax.ShapeDtypeStruct((TWO, 4, LANES, FF_HALF), F32),
            jax.ShapeDtypeStruct((4, LANES, FF_HALF), F32),
            jax.ShapeDtypeStruct((4, LANES, FF_HALF), F32),
            jax.ShapeDtypeStruct((4, 448, WIDTH), F32),
            jax.ShapeDtypeStruct((4, 448, WIDTH), F32),
        ],
        compiler_params=params(3),
        cost_estimate=pl.CostEstimate(flops=30_000_000_000, bytes_accessed=50_000_000, transcendentals=4_000_000),
    )(sc, b_own, b_other, d_all, d_all, ranks, comb_own, comb_other, w_gate, w_up, *pieces, w_down, wd1)


HEAD_COLS = 8192
HEAD_BLOCK = 1024
HEAD_TILE = 1024
HEAD_HALF = 16000
HEAD_SHIFT = 7808
HEAD_OVERLAP = HEAD_COLS - HEAD_SHIFT


def head_start(x, core):
    return x * HEAD_HALF + core * HEAD_SHIFT


def fill_head_weights(sc, own, p1, rx2, ry2, rx3, ry3, w):
    rep = sc[TWO]
    w[ZERO:LANES, :] = own[ALL]
    w[LANES:256, :] = p1[ALL]
    for k, (rx, ry) in ((TWO, (rx2, ry2)), (3, (rx3, ry3))):
        w[pl.ds(pl.multiple_of(k * LANES + rep * 64, 64), 64), :] = rx[ALL]
        w[pl.ds(pl.multiple_of(k * LANES + (ONE - rep) * 64, 64), 64), :] = ry[ALL]


def head_weight_specs():
    return [pl.BlockSpec((LANES, HEAD_BLOCK), lambda i, sc: (ZERO, i))] * TWO + [pl.BlockSpec((64, HEAD_BLOCK), lambda i, sc: (ZERO, i))] * 4


def head_stats_kernel(sc, x_ref, own, p1, rx2, ry2, rx3, ry3, out_ref, w, xp, m_acc, s_acc):
    i = pl.program_id(ZERO)
    rows = x_ref.shape[ZERO]

    @pl.when(i == ZERO)
    def _():
        xp[ALL] = permuted_columns(x_ref, sc[3])
        m_acc[ALL] = jnp.full((rows, LANES), -1e30, F32)
        s_acc[ALL] = jnp.zeros((rows, LANES), F32)

    fill_head_weights(sc, own, p1, rx2, ry2, rx3, ry3, w)
    first_new = jnp.where((sc[ZERO] == ONE) & (i == ZERO), HEAD_OVERLAP, ZERO)
    tiles = [slice(t, t + HEAD_TILE) for t in range(ZERO, rows, HEAD_TILE)]

    def update(tile, logits):
        pieces = []
        for q in range(HEAD_BLOCK // LANES):
            piece = logits[:, q * LANES:(q + ONE) * LANES]
            if q * LANES < HEAD_OVERLAP:
                piece = piece + jnp.where(q * LANES >= first_new, 0.0, -1e30)
            pieces.append(piece)
        peak = m_acc[tile, :]
        top = functools.reduce(jnp.maximum, pieces, peak)
        total = s_acc[tile, :] * jnp.exp(peak - top)
        for piece in pieces:
            total = total + jnp.exp(piece - top)
        m_acc[tile, :] = top
        s_acc[tile, :] = total

    ahead = dot_nn(xp[tiles[ZERO], :], w[ALL])
    for n, tile in enumerate(tiles):
        logits = ahead
        if n + ONE < len(tiles):
            ahead = dot_nn(xp[tiles[n + ONE], :], w[ALL])
        update(tile, logits)

    @pl.when(i == pl.num_programs(ZERO) - ONE)
    def _():
        top = m_acc[ALL]
        highest = jnp.max(top, axis=ONE, keepdims=True)
        out_ref[:, ZERO:ONE] = highest
        out_ref[:, ONE:TWO] = jnp.sum(s_acc[ALL] * jnp.exp(top - highest), axis=ONE, keepdims=True)


def head_stats(sc, x_rows, pieces):
    rows, width = x_rows.shape
    return pl.pallas_call(
        head_stats_kernel,
        grid_spec=pltpu.PrefetchScalarGridSpec(
            num_scalar_prefetch=ONE,
            grid=(HEAD_COLS // HEAD_BLOCK,),
            in_specs=[pl.BlockSpec((rows, width), lambda i, sc: (ZERO, ZERO))] + head_weight_specs(),
            out_specs=pl.BlockSpec((rows, 8), lambda i, sc: (ZERO, ZERO)),
            scratch_shapes=[pltpu.VMEM((width, HEAD_BLOCK), BF16), pltpu.VMEM((rows, width), BF16)] + [pltpu.VMEM((rows, LANES), F32)] * TWO,
        ),
        out_shape=jax.ShapeDtypeStruct((rows, 8), F32),
        compiler_params=params(ONE),
        cost_estimate=pl.CostEstimate(flops=17_000_000_000, bytes_accessed=25_000_000, transcendentals=16_800_000),
    )(sc, x_rows, *pieces)


def head_dx_kernel(sc, x_ref, label_ref, lse_ref, own, p1, rx2, ry2, rx3, ry3, dl_ref, dx_ref, picked_ref, w, xp, dx_acc, picked_acc):
    i = pl.program_id(ZERO)
    core, x, rep, me = sc[ZERO], sc[ONE], sc[TWO], sc[3]
    rows = x_ref.shape[ZERO]
    half = rows // TWO

    @pl.when(i == ZERO)
    def _():
        xp[ALL] = permuted_columns(x_ref, me)
        dx_acc[ALL] = jnp.zeros_like(dx_acc)
        picked_acc[ALL] = jnp.zeros_like(picked_acc)

    fill_head_weights(sc, own, p1, rx2, ry2, rx3, ry3, w)
    start = head_start(x, core) + i * HEAD_BLOCK
    first_new = jnp.where((core == ONE) & (i == ZERO), HEAD_OVERLAP, ZERO)
    cols = lax.broadcasted_iota(jnp.int32, (HEAD_TILE, HEAD_BLOCK), ONE)
    count = half // HEAD_TILE
    tiles = []
    for side in (rep, ONE - rep):
        for t in range(count):
            tiles.append(pl.ds(pl.multiple_of(side * half + t * HEAD_TILE, HEAD_TILE), HEAD_TILE))

    def gradient(tile, logits):
        hit = cols == label_ref[tile, :] - start
        prob = jnp.exp(logits - lse_ref[tile, :])
        picked = jnp.where(hit, logits, 0.0)
        picked_acc[ALL] += sum(jnp.where(q * LANES >= first_new, 1.0, 0.0) * jnp.sum(picked[:, q * LANES:(q + ONE) * LANES].reshape(HEAD_TILE // 8, 8, LANES), axis=ZERO)
                               for q in range(HEAD_BLOCK // LANES))
        d_logits = (jnp.where(hit, prob - 1.0, prob) * (1.0 / rows)).astype(BF16)
        dl_ref[tile, :] = d_logits
        return d_logits

    def project(n, d_logits):
        overlap = d_logits[:, ZERO:HEAD_OVERLAP]
        overlap = jnp.where(first_new == ZERO, overlap.astype(F32), 0.0).astype(BF16)
        masked = jnp.concatenate([overlap, d_logits[:, HEAD_OVERLAP:]], axis=ONE)
        dx_acc[n * HEAD_TILE:(n + ONE) * HEAD_TILE, :] += dot_nt(masked, w[ALL])

    ahead = dot_nn(xp[tiles[ZERO], :], w[ALL])
    for n, tile in enumerate(tiles):
        logits = ahead
        if n + ONE < len(tiles):
            ahead = dot_nn(xp[tiles[n + ONE], :], w[ALL])
        d_logits = gradient(tile, logits)
        if n < count:
            project(n, d_logits)

    @pl.when(i == pl.num_programs(ZERO) - ONE)
    def _():
        for k in range(4):
            dx_ref[:, pl.ds(pl.multiple_of((me ^ k) * LANES, LANES), LANES)] = dx_acc[:, k * LANES:(k + ONE) * LANES]
        picked_ref[ALL] = picked_acc[ALL]


def head_dx(sc, x_rows, labels, lse, pieces):
    rows, width = x_rows.shape
    return pl.pallas_call(
        head_dx_kernel,
        grid_spec=pltpu.PrefetchScalarGridSpec(
            num_scalar_prefetch=ONE,
            grid=(HEAD_COLS // HEAD_BLOCK,),
            in_specs=[
                pl.BlockSpec((rows, width), lambda i, sc: (ZERO, ZERO)),
                pl.BlockSpec((rows, ONE), lambda i, sc: (ZERO, ZERO)),
                pl.BlockSpec((rows, ONE), lambda i, sc: (ZERO, ZERO)),
            ] + head_weight_specs(),
            out_specs=[pl.BlockSpec((rows, HEAD_BLOCK), lambda i, sc: (ZERO, i)), pl.BlockSpec((rows // TWO, width), lambda i, sc: (ZERO, ZERO)),
                       pl.BlockSpec((8, LANES), lambda i, sc: (ZERO, ZERO))],
            scratch_shapes=[pltpu.VMEM((width, HEAD_BLOCK), BF16), pltpu.VMEM((rows, width), BF16), pltpu.VMEM((rows // TWO, width), F32),
                            pltpu.VMEM((8, LANES), F32)],
        ),
        out_shape=[jax.ShapeDtypeStruct((rows, HEAD_COLS), BF16), jax.ShapeDtypeStruct((rows // TWO, width), F32), jax.ShapeDtypeStruct((8, LANES), F32)],
        compiler_params=params(ONE),
        cost_estimate=pl.CostEstimate(flops=26_000_000_000, bytes_accessed=60_000_000, transcendentals=16_800_000),
    )(sc, x_rows, labels, lse, *pieces)


def head_dw_kernel(sc, xt_ref, dl_ref, d0, d1, d2, d3, xt):
    @pl.when(pl.program_id(ZERO) == ZERO)
    def _():
        me, rep = sc[3], sc[TWO]
        for k in range(TWO):
            xt[k * LANES:(k + ONE) * LANES, :] = xt_ref[pl.ds(pl.multiple_of((me ^ k) * LANES, LANES), LANES), :]
        for k in range(TWO, 4):
            xt[LANES + k * 64:192 + k * 64, :] = xt_ref[pl.ds(pl.multiple_of((me ^ k) * LANES + rep * 64, 64), 64), :]

    dw = dot_nn(xt[ALL], dl_ref[ALL])
    d0[ALL] = dw[ZERO:LANES]
    d1[ALL] = dw[LANES:256]
    d2[ALL] = dw[256:320]
    d3[ALL] = dw[320:384]


def head_dw(sc, x_cols, dl):
    width, rows = x_cols.shape
    block = WIDTH
    return pl.pallas_call(
        head_dw_kernel,
        grid_spec=pltpu.PrefetchScalarGridSpec(
            num_scalar_prefetch=ONE,
            grid=(HEAD_COLS // block,),
            in_specs=[
                pl.BlockSpec((width, rows), lambda i, sc: (ZERO, ZERO)),
                pl.BlockSpec((rows, block), lambda i, sc: (ZERO, i)),
            ],
            out_specs=[pl.BlockSpec((LANES, block), lambda i, sc: (ZERO, i))] * TWO + [pl.BlockSpec((64, block), lambda i, sc: (ZERO, i))] * TWO,
            scratch_shapes=[pltpu.VMEM((384, rows), BF16)],
        ),
        out_shape=[jax.ShapeDtypeStruct((LANES, HEAD_COLS), F32)] * TWO + [jax.ShapeDtypeStruct((64, HEAD_COLS), F32)] * TWO,
        compiler_params=params(ONE),
        cost_estimate=pl.CostEstimate(flops=13_000_000_000, bytes_accessed=52_000_000, transcendentals=ZERO),
    )(sc, x_cols, dl)


def update_near_kernel(sc, rate, w_ref, own, p1, *rest):
    out_ref = rest[-ONE]

    @pl.when(pl.program_id(ZERO) == ZERO)
    def _():
        out_ref[ZERO, ZERO] = w_ref[ZERO, ZERO] - rate[ZERO] * own[ZERO, ZERO]

    @pl.when(pl.program_id(ZERO) == ONE)
    def _():
        out_ref[ZERO, ZERO] = w_ref[ZERO, ZERO] - rate[ZERO] * p1[ZERO, ZERO]


def update_far_kernel(sc, rate, w_ref, first2, first3, second2, second3, *rest):
    out_ref = rest[-ONE]

    @pl.when((pl.program_id(ZERO) == ZERO) & (sc[TWO] == sc[4]))
    def _():
        out_ref[ZERO, ZERO] = w_ref[ZERO, ZERO] - rate[ZERO] * first2[ZERO]

    @pl.when((pl.program_id(ZERO) == ZERO) & (sc[TWO] != sc[4]))
    def _():
        out_ref[ZERO, ZERO] = w_ref[ZERO, ZERO] - rate[ZERO] * second2[ZERO]

    @pl.when((pl.program_id(ZERO) == ONE) & (sc[TWO] == sc[4]))
    def _():
        out_ref[ZERO, ZERO] = w_ref[ZERO, ZERO] - rate[ZERO] * first3[ZERO]

    @pl.when((pl.program_id(ZERO) == ONE) & (sc[TWO] != sc[4]))
    def _():
        out_ref[ZERO, ZERO] = w_ref[ZERO, ZERO] - rate[ZERO] * second3[ZERO]


def update_blocks(kernel, sc, rate, layer, near, w, grads, grad_specs, previous):
    def whole(s, j, sc):
        return layer, TWO * j + jnp.where(s == ZERO, sc[ZERO], ONE - sc[ZERO]), ZERO, (sc[ONE] if near else ONE - sc[ONE])

    block = pl.BlockSpec((ONE, ONE, LANES, FF_HALF), whole)
    in_specs = [pl.BlockSpec(memory_space=pltpu.SMEM), block] + grad_specs
    args = [sc, rate, w] + grads
    aliases = {}
    if previous is not None:
        in_specs.append(pl.BlockSpec(memory_space=pl.ANY))
        aliases = {len(args): ZERO}
        args.append(previous)
    return pl.pallas_call(
        kernel,
        grid_spec=pltpu.PrefetchScalarGridSpec(num_scalar_prefetch=ONE, grid=(TWO, 4), in_specs=in_specs, out_specs=block),
        out_shape=jax.ShapeDtypeStruct(w.shape, F32),
        input_output_aliases=aliases,
        compiler_params=params(TWO),
        cost_estimate=pl.CostEstimate(flops=2_000_000, bytes_accessed=11_000_000, transcendentals=ZERO),
    )(*args)


def early(s, j):
    return jnp.where(s == ZERO, j, 3)


def late(s, j):
    return jnp.where(s == ZERO, ZERO, j)


def update_near(sc, rate, layer, matrix, w, own, p1, previous=None):
    specs = [
        pl.BlockSpec((ONE, ONE, LANES, FF_HALF), lambda s, j, sc: (matrix, early(s, j), ZERO, ZERO)),
        pl.BlockSpec((ONE, ONE, LANES, FF_HALF), lambda s, j, sc: (matrix, late(s, j), ZERO, ZERO)),
    ]
    return update_blocks(update_near_kernel, sc, rate, layer, True, w, [own, p1], specs, previous)


def update_far(sc, rate, layer, matrix, w, rx2, ry2, rx3, ry3, previous):
    sc = jnp.concatenate([sc, jnp.full((ONE,), matrix, jnp.int32)])

    def spec(place, by_x):
        def index(s, j, sc):
            return jnp.where((sc[TWO] == sc[4]) == by_x, place(s, j), ZERO), ZERO, ZERO

        return pl.BlockSpec((ONE, LANES, FF_HALF), index)

    specs = [spec(early, True), spec(late, True), spec(early, False), spec(late, False)]
    return update_blocks(update_far_kernel, sc, rate, layer, False, w, [rx2, rx3, ry2, ry3], specs, previous)


def update_down_kernel(sc, rate, w_ref, own, p1, *rest):
    out_ref = rest[-ONE]
    s = pl.program_id(ZERO)

    @pl.when(s == ZERO)
    def _():
        out_ref[ZERO, ZERO] = w_ref[ZERO, ZERO] - rate[ZERO] * own[ZERO]

    @pl.when(s == ONE)
    def _():
        out_ref[ZERO, ZERO] = w_ref[ZERO, ZERO] - rate[ZERO] * p1[ZERO]


def update_down(sc, rate, layer, w, own, p1, previous=None):
    whole = lambda s, j, sc: (layer, TWO * j + jnp.where(s == ZERO, sc[ZERO], ONE - sc[ZERO]), ZERO, ZERO)
    in_specs = [
        pl.BlockSpec(memory_space=pltpu.SMEM),
        pl.BlockSpec((ONE, ONE, 448, WIDTH), whole),
        pl.BlockSpec((ONE, 448, WIDTH), lambda s, j, sc: (jnp.where(s == ZERO, j, 3), ZERO, ZERO)),
        pl.BlockSpec((ONE, 448, WIDTH), lambda s, j, sc: (jnp.where(s == ZERO, ZERO, j), ZERO, ZERO)),
    ]
    args = [sc, rate, w, own, p1]
    aliases = {}
    if previous is not None:
        in_specs.append(pl.BlockSpec(memory_space=pl.ANY))
        aliases = {len(args): ZERO}
        args.append(previous)
    return pl.pallas_call(
        update_down_kernel,
        grid_spec=pltpu.PrefetchScalarGridSpec(
            num_scalar_prefetch=ONE, grid=(TWO, 4), in_specs=in_specs, out_specs=pl.BlockSpec((ONE, ONE, 448, WIDTH), whole),
        ),
        out_shape=jax.ShapeDtypeStruct(w.shape, F32),
        input_output_aliases=aliases,
        compiler_params=params(TWO),
        cost_estimate=pl.CostEstimate(flops=4_000_000, bytes_accessed=22_000_000, transcendentals=ZERO),
    )(*args)


def update_head_kernel(sc, rate, w_ref, own, p1, rx2, ry2, rx3, ry3, out_ref):
    half = pl.program_id(ZERO) // (pl.num_programs(ZERO) // TWO)
    core, x, rep = sc[ZERO], sc[ONE], sc[TWO]
    lr = rate[ZERO]
    blocks = (
        (x, core, own[ALL]),
        (x, ONE - core, p1[ALL]),
        (ONE - x, core, jnp.where(half == rep, rx2[ALL], ry2[ALL])),
        (ONE - x, ONE - core, jnp.where(half == rep, rx3[ALL], ry3[ALL])),
    )
    for bx, bc, grad in blocks:
        cols = pl.ds(pl.multiple_of(head_start(bx, bc), LANES), HEAD_COLS)
        out_ref[:, cols] = w_ref[:, cols] - lr * grad


def update_head(sc, rate, w, own, p1, rx2, ry2, rx3, ry3):
    rows, vocab = w.shape
    step = 16
    count = rows // step
    inner = count // TWO
    return pl.pallas_call(
        update_head_kernel,
        grid_spec=pltpu.PrefetchScalarGridSpec(
            num_scalar_prefetch=ONE,
            grid=(count,),
            in_specs=[
                pl.BlockSpec(memory_space=pltpu.SMEM),
                pl.BlockSpec((step, vocab), lambda i, sc: (i, ZERO)),
                pl.BlockSpec((step, HEAD_COLS), lambda i, sc: (i, ZERO)),
                pl.BlockSpec((step, HEAD_COLS), lambda i, sc: (i, ZERO)),
            ] + [pl.BlockSpec((step, HEAD_COLS), lambda i, sc: (i % inner, ZERO))] * 4,
            out_specs=pl.BlockSpec((step, vocab), lambda i, sc: (i, ZERO)),
        ),
        out_shape=jax.ShapeDtypeStruct(w.shape, F32),
        compiler_params=params(ONE),
        cost_estimate=pl.CostEstimate(flops=8_000_000, bytes_accessed=50_000_000, transcendentals=ZERO),
    )(sc, rate, w, own, p1, rx2, ry2, rx3, ry3)


def update_embedding_kernel(sc, rate, ids_ref, d_ref, w_ref, out_ref):
    rows = w_ref.shape[ZERO]
    first = sc[3] * (pl.num_programs(ZERO) * rows) + pl.program_id(ZERO) * rows
    index = lax.broadcasted_iota(jnp.int32, (rows, ids_ref.shape[ONE]), ZERO) + first
    onehot = jnp.where(index == ids_ref[ALL], 1.0, 0.0).astype(BF16)
    out_ref[ALL] = w_ref[ALL] - rate[ZERO] * dot_nn(onehot, d_ref[ALL])


def update_embedding(sc, rate, ids, d_rows, w):
    rows, width = w.shape
    step = 400
    tokens = d_rows.shape[ZERO]
    return pl.pallas_call(
        update_embedding_kernel,
        grid_spec=pltpu.PrefetchScalarGridSpec(
            num_scalar_prefetch=ONE,
            grid=(rows // step,),
            in_specs=[
                pl.BlockSpec(memory_space=pltpu.SMEM),
                pl.BlockSpec((ONE, tokens), lambda i, sc: (ZERO, ZERO)),
                pl.BlockSpec((tokens, width), lambda i, sc: (ZERO, ZERO)),
                pl.BlockSpec((step, width), lambda i, sc: (i, ZERO)),
            ],
            out_specs=pl.BlockSpec((step, width), lambda i, sc: (i, ZERO)),
        ),
        out_shape=jax.ShapeDtypeStruct(w.shape, F32),
        compiler_params=params(ONE),
        cost_estimate=pl.CostEstimate(flops=17_000_000_000, bytes_accessed=35_000_000, transcendentals=ZERO),
    )(sc, rate, ids, d_rows, w)


def peer_of(rep, me, other_rep, k):
    across = (me, me + ONE - TWO * (me % TWO), (me + TWO) % 4, 3 - me)[k]
    return (ONE - rep if other_rep else rep), across


def exchange_kernel(both, in_ref, out_ref, send_sem, recv_sem):
    rep, me = lax.axis_index(REP), lax.axis_index(FSDP)
    slot = rep * 4 + me if both else me
    peers = [(other, k) for other in ((False, True) if both else (False,)) for k in range(4) if other or k]
    barrier = pltpu.get_barrier_semaphore()
    for other, k in peers:
        pl.semaphore_signal(barrier, inc=ONE, device_id=peer_of(rep, me, other, k), device_id_type=pl.DeviceIdType.MESH)
    pl.semaphore_wait(barrier, len(peers))
    copies = []
    for n, (other, k) in enumerate(peers):
        copy = pltpu.make_async_remote_copy(
            src_ref=in_ref, dst_ref=out_ref.at[slot], send_sem=send_sem.at[n], recv_sem=recv_sem.at[n],
            device_id=peer_of(rep, me, other, k), device_id_type=pl.DeviceIdType.MESH)
        copy.start()
        copies.append(copy)
    out_ref[slot] = in_ref[ALL]
    for copy in copies:
        copy.wait()


def exchange(value, both, collective_id):
    count = 8 if both else 4
    return pl.pallas_call(
        functools.partial(exchange_kernel, both),
        in_specs=[pl.BlockSpec(memory_space=pltpu.VMEM)],
        out_specs=pl.BlockSpec(memory_space=pltpu.VMEM),
        out_shape=jax.ShapeDtypeStruct((count,) + value.shape, value.dtype),
        scratch_shapes=[pltpu.SemaphoreType.DMA((count - ONE,)), pltpu.SemaphoreType.DMA((count - ONE,))],
        compiler_params=pltpu.CompilerParams(collective_id=collective_id, has_side_effects=True),
        cost_estimate=pl.CostEstimate(flops=1_000_000_000, bytes_accessed=100_000, transcendentals=ZERO),
        name="exchange",
    )(value)


def row_major(value):
    return with_layout_constraint(value, Layout(major_to_minor=(ZERO, ONE)))


def to_peer(value, k):
    return lax.ppermute(value, FSDP, [(i, i ^ k) for i in range(4)])


def to_replica(value):
    return lax.ppermute(value, REP, [(ZERO, ONE), (ONE, ZERO)])


def solution(mesh):
    batch_spec = P((REP, FSDP))
    layer_spec = P(None, FSDP)
    expert_spec = P(None, None, FSDP)
    param_specs = (P(FSDP), layer_spec, layer_spec, layer_spec, layer_spec, layer_spec, layer_spec, layer_spec, expert_spec, expert_spec, expert_spec, P(FSDP), P(FSDP))
    in_specs = (batch_spec, batch_spec, batch_spec, P(None, (REP, FSDP)), P()) + param_specs
    out_specs = param_specs + (P(),)

    def train_step(tok_ids, tok_labels, tok_pos, expert_idx, learn_rate, embedding, w_query, w_key, w_value, w_attn_out, g_attn, g_mlp, w_router, w_gate, w_up, w_down, g_final, w_head):
        me = lax.axis_index(FSDP)
        rep = lax.axis_index(REP)
        core, x = me % TWO, me // TWO
        place = jnp.stack([core, x, rep, me]).astype(jnp.int32)
        rate = learn_rate.reshape(ONE)
        layers = w_query.shape[ZERO]
        length = tok_ids.shape[ONE]
        tokens = 8 * length
        cos_tab, sin_tab = rope_tables(tok_pos[ZERO])

        packed = jnp.concatenate([tok_ids, tok_labels, expert_idx[ZERO, ZERO].T, expert_idx[ONE, ZERO].T, tok_ids, tok_labels], axis=ZERO)
        packed = exchange(packed, True, ZERO)
        all_ids, all_labels = packed[:, ZERO].reshape(-ONE), packed[:, ONE].reshape(-ONE, ONE)
        group = tokens // TWO
        chosen_all = [packed[:, TWO + TWO * layer:4 + TWO * layer].transpose(ONE, ZERO, TWO).reshape(TWO, tokens) for layer in range(layers)]
        before = (lax.broadcasted_iota(jnp.int32, (group, group), ZERO) < lax.broadcasted_iota(jnp.int32, (group, group), ONE)).astype(BF16)
        routes = []
        for layer in range(layers):
            experts = lax.broadcasted_iota(jnp.int32, (8, tokens), ZERO)
            mask = ((experts == chosen_all[layer][:ONE]) | (experts == chosen_all[layer][ONE:])).reshape(8, TWO, group).transpose(ONE, ZERO, TWO)
            rank = lax.dot_general(mask.astype(BF16), before, (((TWO,), (ZERO,)), ((), ())), preferred_element_type=F32).astype(jnp.int32)
            rank = jnp.where(mask, rank, -ONE)
            counts = jnp.sum(mask.astype(jnp.int32), axis=TWO).reshape(-ONE)
            routes.append((jnp.concatenate([place, counts]), rank, rank.transpose(ZERO, TWO, ONE)))
        sc = routes[ZERO][ZERO]

        def own_group(values, axis=ZERO):
            return lax.dynamic_slice_in_dim(values, rep * group, group, axis)

        def relay(value, k):
            rx = to_peer(value, k)
            return rx, to_replica(rx)

        def near(value):
            return to_peer(value, ONE)

        def send_experts(layer):
            gu1, mine2, mine3, wd1 = pack_experts(place, layer, w_gate, w_up, w_down)
            pieces = (near(gu1), *relay(mine2, TWO), *relay(mine3, 3))
            return pieces, near(wd1)

        def send_head():
            own, p1, mine2, mine3 = pack_head(place, w_head)
            return [own, near(p1), *relay(mine2, TWO), *relay(mine3, 3)]

        final_col = jnp.stack([g_final, jnp.zeros_like(g_final)])[:, :, None]
        small = jnp.concatenate([w_query, w_key, w_value, w_attn_out, w_router, g_attn[:, :, None], g_mlp[:, :, None], final_col], axis=TWO)
        whole = []
        for layer in range(layers):
            whole.append(lax.all_gather(small[layer].astype(BF16), FSDP, axis=ZERO, tiled=True))
        cuts = (ZERO, WIDTH, 640, 768, 1280, 1288, 1289, 1290, 1291)

        def small_param(layer, slot):
            value = whole[layer][:, cuts[slot]:cuts[slot + ONE]]
            return value[:, ZERO] if slot >= 5 else value

        def attention_params(layer):
            return whole[layer][:, :cuts[3]], whole[layer][:, cuts[3]:cuts[4]], small_param(layer, 5)

        local = own_group(all_ids) - me * embedding.shape[ZERO]
        owned = (local >= ZERO) & (local < embedding.shape[ZERO])
        rows = jnp.take(embedding, jnp.clip(local, ZERO, embedding.shape[ZERO] - ONE), axis=ZERO)
        rows = jnp.where(owned[:, None], rows, 0.0).astype(BF16)
        residual = row_major(lax.psum_scatter(rows, FSDP, scatter_dimension=ZERO, tiled=True).astype(F32))

        sent = [send_experts(layer) for layer in range(layers)]
        head_pieces = send_head()
        saved = []
        for layer in range(layers):
            w_r, gain_m = small_param(layer, 4), small_param(layer, 6)
            residual, attn_vjp = jax.vjp(functools.partial(attention_part, cos_tab=cos_tab, sin_tab=sin_tab), residual, *attention_params(layer))

            def routed(*values, layer=layer):
                return router_part(*values, chosen=expert_idx[layer, ZERO].T)

            (b, _), router_vjp = jax.vjp(routed, residual, gain_m, w_r)
            b_group = lax.all_gather(row_major(b), FSDP, axis=ZERO, tiled=True)
            b_other = to_replica(b_group)
            comb = combine_weights(router_logits(b_group, w_r), own_group(chosen_all[layer], ONE))
            pieces, wd1 = sent[layer]
            partial = expert_forward(sc, layer, b_group, comb.T, w_gate, w_up, pieces, w_down, wd1)
            residual = row_major(residual + lax.psum_scatter(partial, FSDP, scatter_dimension=ZERO, tiled=True))
            saved.append((attn_vjp, router_vjp, b_group, b_other, comb, w_r))

        others, residual = lax.optimization_barrier(([entry[3] for entry in saved], residual))
        comb_others = []
        for layer in range(layers):
            other = lax.dynamic_slice_in_dim(chosen_all[layer], (ONE - rep) * group, group, ONE)
            comb_others.append(combine_weights(router_logits(others[layer], saved[layer][5]), other))
        final, final_vjp = jax.vjp(rms_norm, residual, small_param(ZERO, 7))
        x_all = lax.all_gather(row_major(final), (REP, FSDP), axis=ZERO, tiled=True)
        stats = head_stats(sc, x_all, head_pieces)
        stats = exchange(stats.T, False, ONE)
        peak = jnp.max(stats[:, ZERO], axis=ZERO)
        lse = peak + jnp.log(jnp.sum(stats[:, ONE] * jnp.exp(stats[:, ZERO] - peak), axis=ZERO))
        dl, dx, picked = head_dx(sc, x_all, all_labels, lse[:, None], head_pieces)
        dh0, dh1, dh2, dh3 = head_dw(sc, x_all.T, dl)
        d_final = row_major(lax.psum_scatter(dx, FSDP, scatter_dimension=ZERO, tiled=True))
        d_residual, d_gain_final = final_vjp(d_final.astype(BF16))
        head_returns = [near(dh1), *relay(dh2, TWO), *relay(dh3, 3)]
        new_head = update_head(sc, rate, w_head, dh0, *head_returns)

        small_grads = [None] * layers
        new_gate = new_up = new_down = None
        for layer in reversed(range(layers)):
            attn_vjp, router_vjp, b_group, _, comb, _ = saved[layer]
            d_all = lax.all_gather(row_major(d_residual), (REP, FSDP), axis=ZERO, tiled=True)
            pieces, wd1 = sent[layer]
            scalars, ranks, rank_cols = routes[layer]
            db = expert_dgrad(scalars, layer, b_group, d_all, ranks, rank_cols, comb, w_gate, w_up, pieces, w_down, wd1)
            own, near1, far2, far3, down_own, down_other = expert_wgrad(scalars, layer, b_group, others[layer], d_all, ranks, comb, comb_others[layer], w_gate, w_up, pieces, w_down, wd1)
            returned = (*relay(far2, TWO), *relay(far3, 3))
            gu1 = near(near1)
            down1 = near(down_other)
            new_gate = update_near(place, rate, layer, ZERO, w_gate, own, gu1, new_gate)
            new_up = update_near(place, rate, layer, ONE, w_up, own, gu1, new_up)
            new_gate = update_far(place, rate, layer, ZERO, w_gate, *returned, new_gate)
            new_up = update_far(place, rate, layer, ONE, w_up, *returned, new_up)
            new_down = update_down(sc, rate, layer, w_down, down_own, down1, previous=new_down)
            db = row_major(lax.psum_scatter(db, FSDP, scatter_dimension=ZERO, tiled=True))
            d_router_in, d_gain_m, d_wr = router_vjp((db[:, :WIDTH].astype(BF16), db[:, WIDTH:520].T))
            d_residual = d_residual + d_router_in
            d_residual, d_wqkv, d_wo, d_gain_a = attn_vjp(d_residual)
            extra = d_gain_final if layer == ZERO else jnp.full_like(d_gain_final, ZERO, F32) + jnp.sum(picked)
            grads = [d_wqkv, d_wo, d_wr, d_gain_a[:, None], d_gain_m[:, None], extra[:, None]]
            grads = jnp.concatenate([g.astype(F32) for g in grads], axis=ONE)
            if layer + ONE < layers:
                grads, small_grads[layer + ONE] = lax.optimization_barrier((grads, small_grads[layer + ONE]))
            grads = lax.psum_scatter(grads, FSDP, scatter_dimension=ZERO, tiled=True)
            small_grads[layer] = lax.psum(grads, REP)

        d_rows = lax.all_gather(row_major(d_residual.astype(BF16)), (REP, FSDP), axis=ZERO, tiled=True)
        new_embedding = update_embedding(sc, rate, all_ids[None, :], d_rows, embedding)

        small_grad = jnp.stack(small_grads)
        new_small = small - learn_rate * small_grad
        mean_loss = (jnp.sum(lse) - small_grad[ONE, ZERO, 1290] / TWO) / tokens

        def new_param(slot):
            value = new_small[:, :, cuts[slot]:cuts[slot + ONE]]
            return value[:, :, ZERO] if slot >= 5 else value

        return (new_embedding, new_param(ZERO), new_param(ONE), new_param(TWO), new_param(3), new_param(5), new_param(6), new_param(4),
                new_gate, new_up, new_down, new_param(7)[ZERO], new_head, mean_loss)


    return jax.shard_map(train_step, mesh=mesh, in_specs=in_specs, out_specs=out_specs, check_vma=False)
```

```python
import functools
import jax
import jax.numpy as jnp
from jax import lax
from jax.experimental import pallas as pl
from jax.experimental.pallas import tpu as pltpu
from jax.experimental.layout import Layout, with_layout_constraint
from jax.sharding import PartitionSpec as P

ZERO, ONE, TWO, ALL = 0, 1, 2, ...
LANES = 128
WIDTH = 512
FF_HALF = 896
HEAD_DIM = LANES
ROPE_THETA = 1000000.0
NORM_EPS = 1e-5
BF16 = jnp.bfloat16
F32 = jnp.float32
VMEM_LIMIT = 60 * 1024 * 1024
FSDP = 'fsdp'
REP = 'rep'


def rms_norm(residual, gain):
    mean_sq = jnp.mean(residual * residual, axis=-ONE, keepdims=True)
    return (residual * lax.rsqrt(mean_sq + NORM_EPS) * gain).astype(BF16)


def rope_tables(positions):
    inv_freq = ROPE_THETA ** (-jnp.arange(ZERO, HEAD_DIM, TWO, dtype=F32) / HEAD_DIM)
    angle = positions.astype(F32)[ALL, None] * inv_freq
    return jnp.cos(angle)[:, None, :], jnp.sin(angle)[:, None, :]


def apply_rope(heads, cos_tab, sin_tab):
    half_dim = heads.shape[-ONE] // TWO
    lower = heads[ALL, :half_dim]
    upper = heads[ALL, half_dim:]
    return jnp.concatenate([lower * cos_tab - upper * sin_tab, upper * cos_tab + lower * sin_tab], axis=-ONE)


def attention_part(residual, w_qkv, w_o, gain, cos_tab, sin_tab):
    length = residual.shape[ZERO]
    q_width = w_o.shape[ZERO]
    q_heads = q_width // HEAD_DIM
    normed = rms_norm(residual, gain)
    projected = jnp.dot(normed, w_qkv, preferred_element_type=F32)
    values = projected[:, q_width + HEAD_DIM:].astype(BF16)
    turned = apply_rope(projected[:, :q_width + HEAD_DIM].reshape(length, q_heads + ONE, HEAD_DIM), cos_tab, sin_tab).astype(BF16)
    query, keyed = turned[:, :q_heads], turned[:, q_heads]
    scores = jnp.einsum('qgd,sd->gqs', query, keyed, preferred_element_type=F32) * HEAD_DIM ** -0.5
    causal = lax.broadcasted_iota(jnp.int32, (length, length), ZERO) >= lax.broadcasted_iota(jnp.int32, (length, length), ONE)
    scores = jnp.where(causal, scores, -1e30)
    attn_probs = jax.nn.softmax(scores, axis=-ONE).astype(BF16)
    mixed = jnp.einsum('gqs,sd->qgd', attn_probs, values, preferred_element_type=F32).astype(BF16)
    mixed = mixed.reshape(length, q_width)
    return residual + jnp.dot(mixed, w_o, preferred_element_type=F32)


def combine_weights(logits, chosen):
    rows = lax.broadcasted_iota(jnp.int32, logits.shape, ZERO)
    first = rows == chosen[:ONE]
    second = rows == chosen[ONE:]
    r0 = jnp.sum(jnp.where(first, logits, 0.0), axis=ZERO, keepdims=True)
    r1 = jnp.sum(jnp.where(second, logits, 0.0), axis=ZERO, keepdims=True)
    gates = jax.nn.softmax(jnp.concatenate([r0, r1], axis=ZERO), axis=ZERO)
    return jnp.where(first, gates[:ONE], 0.0) + jnp.where(second, gates[ONE:], 0.0)


def router_logits(normed, w_r):
    return lax.dot_general(w_r, normed, (((ZERO,), (ONE,)), ((), ())), preferred_element_type=F32)


def dot_tn(a, b):
    return dot_nn(a.T.astype(BF16), b)


def norm_backward(value, gain, d_out):
    width = value.shape[ONE]
    inverse = lax.rsqrt(jnp.mean(value * value, axis=ONE, keepdims=True) + NORM_EPS)
    unit = value * inverse
    scaled = d_out * gain
    along = jnp.sum(scaled * unit, axis=ONE, keepdims=True) / width
    return inverse * (scaled - unit * along), jnp.sum(d_out * unit, axis=ZERO, keepdims=True)


def normalize(value, gain):
    return value * lax.rsqrt(jnp.mean(value * value, axis=ONE, keepdims=True) + NORM_EPS) * gain


def round_trip(value):
    return value.astype(BF16).astype(F32)


def block_backward_kernel(r0_ref, r1_ref, dr_ref, db_ref, whole_ref, gain_ref, cos_ref, sin_ref, chosen_ref, extra_ref, d_ref, grad_ref):
    tokens, width = r0_ref.shape
    gain_a = gain_ref[ZERO:ONE, :].astype(F32)
    gain_m = gain_ref[ONE:TWO, :].astype(F32)
    r1 = r1_ref[ALL]
    b = normalize(r1, gain_m)
    w_r = whole_ref[:, 1280:1408]
    logits = dot_nn(b.astype(BF16), w_r)
    lanes = lax.broadcasted_iota(jnp.int32, (tokens, LANES), ONE)
    first = lanes == chosen_ref[:, ZERO:ONE]
    second = lanes == chosen_ref[:, ONE:TWO]

    def pick(mask, value):
        return jnp.sum(jnp.where(mask, value, 0.0), axis=ONE, keepdims=True)

    l0, l1 = pick(first, logits), pick(second, logits)
    top = jnp.maximum(l0, l1)
    e0, e1 = jnp.exp(l0 - top), jnp.exp(l1 - top)
    g0, g1 = e0 / (e0 + e1), e1 / (e0 + e1)
    d_comb = db_ref[:, width:width + LANES]
    d0, d1 = pick(first, d_comb), pick(second, d_comb)
    shared = g0 * d0 + g1 * d1
    d_logits = (jnp.where(first, g0 * (d0 - shared), 0.0) + jnp.where(second, g1 * (d1 - shared), 0.0)).astype(BF16)
    d_b = round_trip(round_trip(db_ref[:, ZERO:width]) + round_trip(dot_nt(d_logits, w_r)))
    d_wr = dot_tn(round_trip(b), d_logits)
    d_value, d_gain_m = norm_backward(r1, gain_m, d_b)
    dr = dr_ref[ALL] + d_value
    r0 = r0_ref[ALL]
    a = normalize(r0, gain_a)
    w_qkv = whole_ref[:, ZERO:768]
    projected = dot_nn(a.astype(BF16), w_qkv)
    cos, sin = cos_ref[ALL], sin_ref[ALL]

    def turn(value):
        return value * cos + pltpu.roll(value, 64, ONE) * sin

    def turn_back(value):
        return value * cos + pltpu.roll(value * sin, 64, ONE)

    keyed = turn(projected[:, WIDTH:640]).astype(BF16)
    values = projected[:, 640:768].astype(BF16)
    allowed = lax.broadcasted_iota(jnp.int32, (tokens, tokens), ZERO) >= lax.broadcasted_iota(jnp.int32, (tokens, tokens), ONE)
    scale = HEAD_DIM ** -0.5
    dr_low = dr.astype(BF16)
    d_mixed = dot_nt(dr_low, whole_ref[:, 768:1280]).astype(BF16)
    d_keyed = jnp.zeros((tokens, LANES), F32)
    d_values = jnp.zeros((tokens, LANES), F32)
    d_projected, mixed = [], []
    for head in range(4):
        cols = slice(head * LANES, head * LANES + LANES)
        query = turn(projected[:, cols])
        scores = jnp.where(allowed, dot_nt(query.astype(BF16), keyed) * scale, -1e30)
        weight = jnp.exp(scores - jnp.max(scores, axis=ONE, keepdims=True))
        weight = weight / jnp.sum(weight, axis=ONE, keepdims=True)
        rounded = round_trip(weight)
        mixed.append(round_trip(dot_nn(rounded.astype(BF16), values)))
        d_out = d_mixed[:, cols]
        d_weight = round_trip(dot_nt(d_out, values))
        d_values += dot_tn(rounded, d_out)
        d_scores = weight * (d_weight - jnp.sum(d_weight * weight, axis=ONE, keepdims=True)) * scale
        d_projected.append(turn_back(round_trip(dot_nn(d_scores.astype(BF16), keyed))))
        d_keyed += dot_tn(d_scores, query.astype(BF16))
    d_projected = jnp.concatenate(d_projected + [turn_back(round_trip(d_keyed)), round_trip(d_values)], axis=ONE).astype(BF16)
    grad_ref[:, ZERO:768] = dot_tn(round_trip(a), d_projected)
    grad_ref[:, 768:1280] = dot_tn(jnp.concatenate(mixed, axis=ONE), dr_low)
    d_value, d_gain_a = norm_backward(r0, gain_a, round_trip(dot_nt(d_projected, w_qkv)))
    d_ref[ALL] = dr + d_value
    row = lax.broadcasted_iota(jnp.int32, (LANES, width), ZERO)
    gains = jnp.where(row == 8, d_gain_a, jnp.where(row == 9, d_gain_m, jnp.where(row == 10, extra_ref[ALL], 0.0)))
    grad_ref[:, 1280:1408] = d_wr + gains.T


def block_backward(r0, r1, d_residual, db, whole, gains, cos, sin, chosen, extra):
    tokens, width = r0.shape
    return pl.pallas_call(
        block_backward_kernel,
        out_shape=[jax.ShapeDtypeStruct((tokens, width), F32), jax.ShapeDtypeStruct((width, 1408), F32)],
        compiler_params=pltpu.CompilerParams(vmem_limit_bytes=VMEM_LIMIT),
        cost_estimate=pl.CostEstimate(flops=2_000_000_000, bytes_accessed=8_000_000, transcendentals=300_000),
    )(r0, r1, d_residual, db, whole, gains, cos, sin, chosen, extra)


def dot_nn(a, b):
    return jnp.dot(a, b, preferred_element_type=F32)


def dot_nt(a, b):
    return lax.dot_general(a, b, (((ONE,), (ONE,)), ((), ())), preferred_element_type=F32)


def params(steps):
    return pltpu.CompilerParams(dimension_semantics=("arbitrary",) * steps, vmem_limit_bytes=VMEM_LIMIT)


def permuted_columns(ref, me):
    return jnp.concatenate([ref[:, pl.ds(pl.multiple_of((me ^ k) * LANES, LANES), LANES)] for k in range(4)], axis=ONE)


def pack_experts_kernel(sc, gate1, up1, gate2, up2, gate3, up3, down1, out1, out2, out3, out_down):
    rep = sc[TWO]
    out1[ZERO, ZERO] = gate1[ZERO, ZERO].astype(BF16)
    out1[ONE, ZERO] = up1[ZERO, ZERO].astype(BF16)
    out2[ZERO] = jnp.where(rep == ZERO, gate2[ZERO, ZERO], up2[ZERO, ZERO]).astype(BF16)
    out3[ZERO] = jnp.where(rep == ZERO, gate3[ZERO, ZERO], up3[ZERO, ZERO]).astype(BF16)
    out_down[ZERO] = down1[ZERO, ZERO].astype(BF16)


def pack_experts(sc, layer, w_gate, w_up, w_down):
    def spec(own_core, own_half, matrix=None):
        def index(j, sc):
            step = j if matrix is None else jnp.where(sc[TWO] == matrix, j, ZERO)
            core = sc[ZERO] if own_core else ONE - sc[ZERO]
            return layer, TWO * step + core, ZERO, (sc[ONE] if own_half else ONE - sc[ONE])

        return pl.BlockSpec((ONE, ONE, LANES, FF_HALF), index)

    block = lambda j, sc: (j, ZERO, ZERO)
    return pl.pallas_call(
        pack_experts_kernel,
        grid_spec=pltpu.PrefetchScalarGridSpec(
            num_scalar_prefetch=ONE,
            grid=(4,),
            in_specs=[spec(False, True), spec(False, True), spec(True, False, ZERO), spec(True, False, ONE), spec(False, False, ZERO), spec(False, False, ONE),
                      pl.BlockSpec((ONE, ONE, 448, WIDTH), lambda j, sc: (layer, TWO * j + ONE - sc[ZERO], ZERO, ZERO))],
            out_specs=[pl.BlockSpec((TWO, ONE, LANES, FF_HALF), lambda j, sc: (ZERO, j, ZERO, ZERO)), pl.BlockSpec((ONE, LANES, FF_HALF), block), pl.BlockSpec((ONE, LANES, FF_HALF), block),
                       pl.BlockSpec((ONE, 448, WIDTH), block)],
        ),
        out_shape=[
            jax.ShapeDtypeStruct((TWO, 4, LANES, FF_HALF), BF16),
            jax.ShapeDtypeStruct((4, LANES, FF_HALF), BF16),
            jax.ShapeDtypeStruct((4, LANES, FF_HALF), BF16),
            jax.ShapeDtypeStruct((4, 448, WIDTH), BF16),
        ],
        compiler_params=params(ONE),
        cost_estimate=pl.CostEstimate(flops=10_000_000, bytes_accessed=17_000_000, transcendentals=ZERO),
    )(sc, w_gate, w_up, w_gate, w_up, w_gate, w_up, w_down)


def pack_head_kernel(sc, w_ref, out0, out1, out2, out3):
    core, x, rep = sc[ZERO], sc[ONE], sc[TWO]

    def part(xx, cc):
        return w_ref[:, pl.ds(pl.multiple_of(head_start(xx, cc), LANES), HEAD_COLS)].astype(BF16)

    out0[ALL] = part(x, core)
    out1[ALL] = part(x, ONE - core)

    @pl.when(pl.program_id(ZERO) // (pl.num_programs(ZERO) // TWO) == rep)
    def _():
        out2[ALL] = part(ONE - x, core)
        out3[ALL] = part(ONE - x, ONE - core)


def pack_head(sc, w):
    rows, vocab = w.shape
    step = 16
    count = rows // step
    half = lambda i, sc: (jnp.clip(i - sc[TWO] * (count // TWO), ZERO, count // TWO - ONE), ZERO)
    return pl.pallas_call(
        pack_head_kernel,
        grid_spec=pltpu.PrefetchScalarGridSpec(
            num_scalar_prefetch=ONE,
            grid=(count,),
            in_specs=[pl.BlockSpec((step, vocab), lambda i, sc: (i, ZERO))],
            out_specs=[pl.BlockSpec((step, HEAD_COLS), lambda i, sc: (i, ZERO))] * TWO + [pl.BlockSpec((step, HEAD_COLS), half)] * TWO,
        ),
        out_shape=[jax.ShapeDtypeStruct((rows, HEAD_COLS), BF16)] * TWO + [jax.ShapeDtypeStruct((rows // TWO, HEAD_COLS), BF16)] * TWO,
        compiler_params=params(ONE),
        cost_estimate=pl.CostEstimate(flops=10_000_000, bytes_accessed=23_000_000, transcendentals=ZERO),
    )(sc, w)


def fill_expert_weights(sc, wg_own, wu_own, gu1, rx2, ry2, rx3, ry3, wd_own, wd1, wgu, wd):
    core, rep = sc[ZERO], sc[TWO]
    wgu[ZERO:LANES, ZERO:FF_HALF] = wg_own[ZERO, ZERO].astype(BF16)
    wgu[ZERO:LANES, FF_HALF:1792] = wu_own[ZERO, ZERO].astype(BF16)
    wgu[LANES:256, ZERO:FF_HALF] = gu1[ZERO, ZERO]
    wgu[LANES:256, FF_HALF:1792] = gu1[ONE, ZERO]
    by_x = pl.ds(pl.multiple_of(rep * FF_HALF, LANES), FF_HALF)
    by_y = pl.ds(pl.multiple_of((ONE - rep) * FF_HALF, LANES), FF_HALF)
    wgu[256:384, by_x] = rx2[ZERO]
    wgu[384:WIDTH, by_x] = rx3[ZERO]
    wgu[256:384, by_y] = ry2[ZERO]
    wgu[384:WIDTH, by_y] = ry3[ZERO]
    wd[pl.ds(pl.multiple_of(core * 448, 64), 448), :] = wd_own[ZERO, ZERO].astype(BF16)
    wd[pl.ds(pl.multiple_of((ONE - core) * 448, 64), 448), :] = wd1[ZERO]


def expert_weight_specs(layer):
    own = lambda j, t, sc: (layer, TWO * j + sc[ZERO], ZERO, sc[ONE])
    return [
        pl.BlockSpec((ONE, ONE, LANES, FF_HALF), own),
        pl.BlockSpec((ONE, ONE, LANES, FF_HALF), own),
        pl.BlockSpec((TWO, ONE, LANES, FF_HALF), lambda j, t, sc: (ZERO, j, ZERO, ZERO)),
        pl.BlockSpec((ONE, LANES, FF_HALF), lambda j, t, sc: (j, ZERO, ZERO)),
        pl.BlockSpec((ONE, LANES, FF_HALF), lambda j, t, sc: (j, ZERO, ZERO)),
        pl.BlockSpec((ONE, LANES, FF_HALF), lambda j, t, sc: (j, ZERO, ZERO)),
        pl.BlockSpec((ONE, LANES, FF_HALF), lambda j, t, sc: (j, ZERO, ZERO)),
        pl.BlockSpec((ONE, ONE, 448, WIDTH), lambda j, t, sc: (layer, TWO * j + sc[ZERO], ZERO, ZERO)),
        pl.BlockSpec((ONE, 448, WIDTH), lambda j, t, sc: (j, ZERO, ZERO)),
    ]


EXPERT_SCRATCH = [pltpu.VMEM((WIDTH, 1792), BF16), pltpu.VMEM((FF_HALF, WIDTH), BF16)]


def expert_column(comb, expert):
    lanes = lax.broadcasted_iota(jnp.int32, comb.shape, ONE)
    return jnp.sum(jnp.where(lanes == expert, comb, 0.0), axis=ONE, keepdims=True)


def expert_forward_kernel(sc, b_ref, comb_ref, wg_own, wu_own, gu1, rx2, ry2, rx3, ry3, wd_own, wd1, out_ref, wgu, wd):
    j, t = pl.program_id(ZERO), pl.program_id(ONE)
    tile = b_ref.shape[ZERO]

    @pl.when(t == ZERO)
    def _():
        fill_expert_weights(sc, wg_own, wu_own, gu1, rx2, ry2, rx3, ry3, wd_own, wd1, wgu, wd)

    b = permuted_columns(b_ref, sc[3])
    both = dot_nn(b, wgu[ALL])
    gate, up = both[:, ZERO:FF_HALF], both[:, FF_HALF:1792]
    hidden = (gate * jax.nn.sigmoid(gate) * up).astype(BF16)
    weighted = dot_nn(hidden, wd[ALL]) * expert_column(comb_ref[ALL], TWO * j + sc[ZERO])
    rows = pl.ds(pl.multiple_of(t * tile, tile), tile)

    @pl.when(j == ZERO)
    def _():
        out_ref[rows, :] = weighted

    @pl.when(j != ZERO)
    def _():
        out_ref[rows, :] += weighted


def expert_forward(sc, layer, b_rows, comb, w_gate, w_up, pieces, w_down, wd1):
    rows, width = b_rows.shape
    tile = 1024
    return pl.pallas_call(
        expert_forward_kernel,
        grid_spec=pltpu.PrefetchScalarGridSpec(
            num_scalar_prefetch=ONE,
            grid=(4, rows // tile),
            in_specs=[
                pl.BlockSpec((tile, width), lambda j, t, sc: (t, ZERO)),
                pl.BlockSpec((tile, 8), lambda j, t, sc: (t, ZERO)),
            ] + expert_weight_specs(layer),
            out_specs=pl.BlockSpec((rows, width), lambda j, t, sc: (ZERO, ZERO)),
            scratch_shapes=EXPERT_SCRATCH,
        ),
        out_shape=jax.ShapeDtypeStruct((rows, width), F32),
        compiler_params=params(TWO),
        cost_estimate=pl.CostEstimate(flops=11_300_000_000, bytes_accessed=20_000_000, transcendentals=3_700_000),
    )(sc, b_rows, comb, w_gate, w_up, *pieces, w_down, wd1)


SLOT_TILE = 256


def slot_gradients(b_sel, d_sel, weight, wgu, wd):
    both = dot_nn(b_sel, wgu[ALL])
    gate, up = both[:, ZERO:FF_HALF], both[:, FF_HALF:1792]
    sig = jax.nn.sigmoid(gate)
    silu = gate * sig
    hidden = (silu * up).astype(BF16).astype(F32)
    d_hidden = dot_nt(d_sel, wd[ALL])
    d_weight = jnp.sum(hidden * d_hidden, axis=ONE, keepdims=True)
    d_hidden = (d_hidden * weight).astype(BF16).astype(F32)
    d_up = (d_hidden * silu).astype(BF16)
    d_gate = (d_hidden * up * (sig * (1.0 + gate * (1.0 - sig)))).astype(BF16)
    return (hidden * weight).astype(BF16), jnp.concatenate([d_gate, d_up], axis=ONE), d_weight


def load_tokens(rows_ref, b_ref, d_ref, me):
    rows_ref[:, ZERO:WIDTH] = permuted_columns(b_ref, me)
    rows_ref[:, WIDTH:1024] = d_ref[ALL].astype(BF16)


def select_slots(rank_row, comb_row, m, tokens_ref):
    index = lax.broadcasted_iota(jnp.int32, (SLOT_TILE, rank_row.shape[ONE]), ZERO) + m * SLOT_TILE
    chosen = index == rank_row
    picked = dot_nn(jnp.where(chosen, 1.0, 0.0).astype(BF16), tokens_ref[ALL])
    weight = jnp.sum(jnp.where(chosen, comb_row, 0.0), axis=ONE, keepdims=True)
    return chosen, picked[:, ZERO:WIDTH], picked[:, WIDTH:1024], weight


def slot_tiles(sc, group, expert):
    return (sc[4 + group * 8 + expert] + (SLOT_TILE - ONE)) // SLOT_TILE


def expert_dgrad_kernel(sc, b_ref, d_ref, rank_ref, rank_col_ref, comb_ref, wg_own, wu_own, gu1, rx2, ry2, rx3, ry3, wd_own, wd1,
                        db_ref, wgu, wd, tokens_ref, db_acc, dw_acc):
    j = pl.program_id(ZERO)
    core, rep, me = sc[ZERO], sc[TWO], sc[3]
    expert = TWO * j + core

    @pl.when(j == ZERO)
    def _():
        load_tokens(tokens_ref, b_ref, d_ref, me)
        db_acc[ALL] = jnp.zeros_like(db_acc)
        dw_acc[ALL] = jnp.zeros_like(dw_acc)

    fill_expert_weights(sc, wg_own, wu_own, gu1, rx2, ry2, rx3, ry3, wd_own, wd1, wgu, wd)

    row = pl.ds(expert, ONE)

    def slots(m, carry):
        chosen, b_sel, d_sel, weight = select_slots(rank_ref[ZERO, row, :], comb_ref[row, :], m, tokens_ref)
        _, d_both, d_weight = slot_gradients(b_sel.astype(BF16), d_sel.astype(BF16), weight, wgu, wd)
        db = dot_nt(d_both, wgu[ALL])
        high = db.astype(BF16)
        rest = db - high.astype(F32)
        middle = rest.astype(BF16)
        low = (rest - middle.astype(F32)).astype(BF16)
        rank_all = rank_col_ref[ZERO]
        lanes = lax.broadcasted_iota(jnp.int32, rank_all.shape, ONE)
        rank_col = jnp.sum(jnp.where(lanes == expert, rank_all, ZERO), axis=ONE, keepdims=True)
        index = lax.broadcasted_iota(jnp.int32, (rank_all.shape[ZERO], SLOT_TILE), ONE) + m * SLOT_TILE
        spread = jnp.where(index == rank_col, 1.0, 0.0).astype(BF16)
        db_acc[ALL] += dot_nn(jnp.concatenate([spread] * 3, axis=ONE), jnp.concatenate([high, middle, low], axis=ZERO))
        dw_acc[row, :] += jnp.sum(jnp.where(chosen, d_weight, 0.0), axis=ZERO, keepdims=True)
        return carry

    lax.fori_loop(ZERO, slot_tiles(sc, rep, expert), slots, ZERO)

    @pl.when(j == pl.num_programs(ZERO) - ONE)
    def _():
        for k in range(4):
            db_ref[:, pl.ds(pl.multiple_of((me ^ k) * LANES, LANES), LANES)] = db_acc[:, k * LANES:(k + ONE) * LANES]
        db_ref[:, WIDTH:640] = dw_acc[ALL].T


def expert_dgrad(sc, layer, b_group, d_all, ranks, rank_cols, comb, w_gate, w_up, pieces, w_down, wd1):
    rows, width = b_group.shape
    return pl.pallas_call(
        expert_dgrad_kernel,
        grid_spec=pltpu.PrefetchScalarGridSpec(
            num_scalar_prefetch=ONE,
            grid=(4, ONE),
            in_specs=[
                pl.BlockSpec((rows, width), lambda j, t, sc: (ZERO, ZERO)),
                pl.BlockSpec((rows, width), lambda j, t, sc: (sc[TWO], ZERO)),
                pl.BlockSpec((ONE, 8, rows), lambda j, t, sc: (sc[TWO], ZERO, ZERO)),
                pl.BlockSpec((ONE, rows, 8), lambda j, t, sc: (sc[TWO], ZERO, ZERO)),
                pl.BlockSpec((8, rows), lambda j, t, sc: (ZERO, ZERO)),
            ] + expert_weight_specs(layer),
            out_specs=pl.BlockSpec((rows, 640), lambda j, t, sc: (ZERO, ZERO)),
            scratch_shapes=EXPERT_SCRATCH + [pltpu.VMEM((rows, TWO * width), BF16), pltpu.VMEM((rows, width), F32), pltpu.VMEM((LANES, rows), F32)],
        ),
        out_shape=jax.ShapeDtypeStruct((rows, 640), F32),
        compiler_params=params(TWO),
        cost_estimate=pl.CostEstimate(flops=15_000_000_000, bytes_accessed=25_000_000, transcendentals=2_000_000),
    )(sc, b_group, d_all, ranks, rank_cols, comb, w_gate, w_up, *pieces, w_down, wd1)


def expert_wgrad_kernel(sc, b_own, b_other, d_own, d_other, rank_ref, comb_own, comb_other,
                        wg_own, wu_own, gu1, rx2, ry2, rx3, ry3, wd_own, wd1,
                        own_ref, near_ref, far2_ref, far3_ref, down_own_ref, down_other_ref, wgu, wd, tokens_ref, comb_ref, down_acc):
    j, group = pl.program_id(ZERO), pl.program_id(ONE)
    core, rep, me = sc[ZERO], sc[TWO], sc[3]
    expert = TWO * j + core

    @pl.when((j == ZERO) & (group == ZERO))
    def _():
        load_tokens(tokens_ref.at[rep], b_own, d_own, me)
        load_tokens(tokens_ref.at[ONE - rep], b_other, d_other, me)
        comb_ref[rep] = comb_own[ALL]
        comb_ref[ONE - rep] = comb_other[ALL]

    @pl.when(group == ZERO)
    def _():
        fill_expert_weights(sc, wg_own, wu_own, gu1, rx2, ry2, rx3, ry3, wd_own, wd1, wgu, wd)
        for ref in (own_ref, near_ref, far2_ref, far3_ref, down_acc):
            ref[ALL] = jnp.zeros_like(ref)

    row = pl.ds(expert, ONE)

    def slots(m, carry):
        _, b_sel, d_sel, weight = select_slots(rank_ref[ZERO, row, :], comb_ref[group, row, :], m, tokens_ref.at[group])
        hidden, d_both, _ = slot_gradients(b_sel.astype(BF16), d_sel.astype(BF16), weight, wgu, wd)
        bt = b_sel.T.astype(BF16)
        dt = d_sel.T.astype(BF16)
        dw = dot_nn(bt[ZERO:256], d_both)
        for matrix in range(TWO):
            cols = slice(matrix * FF_HALF, matrix * FF_HALF + FF_HALF)
            own_ref[matrix, ZERO] += dw[ZERO:LANES, cols]
            near_ref[matrix, ZERO] += dw[LANES:256, cols]
        dw = dot_nn(bt[256:WIDTH], jnp.where(rep == ZERO, d_both[:, ZERO:FF_HALF], d_both[:, FF_HALF:1792]))
        far2_ref[ZERO] += dw[ZERO:LANES]
        far3_ref[ZERO] += dw[LANES:256]
        down_acc[ALL] += dot_nn(dt, hidden)
        return carry

    lax.fori_loop(ZERO, slot_tiles(sc, group, expert), slots, ZERO)

    @pl.when(group == ONE)
    def _():
        down_t = down_acc[ALL].T
        lower, upper = down_t[ZERO:448], down_t[448:FF_HALF]

        @pl.when(core == ZERO)
        def _():
            down_own_ref[ZERO] = lower
            down_other_ref[ZERO] = upper

        @pl.when(core != ZERO)
        def _():
            down_own_ref[ZERO] = upper
            down_other_ref[ZERO] = lower


def expert_wgrad(sc, layer, b_own, b_other, d_all, ranks, comb_own, comb_other, w_gate, w_up, pieces, w_down, wd1):
    rows, width = b_own.shape
    once = pl.BlockSpec((rows, width), lambda j, g, t, sc: (ZERO, ZERO))
    weights = [pl.BlockSpec(spec.block_shape, functools.partial(lambda index, j, g, t, sc: index(j, t, sc), spec.index_map)) for spec in expert_weight_specs(layer)]
    return pl.pallas_call(
        expert_wgrad_kernel,
        grid_spec=pltpu.PrefetchScalarGridSpec(
            num_scalar_prefetch=ONE,
            grid=(4, TWO, ONE),
            in_specs=[once] * TWO + [
                pl.BlockSpec((rows, width), lambda j, g, t, sc: (sc[TWO], ZERO)),
                pl.BlockSpec((rows, width), lambda j, g, t, sc: (ONE - sc[TWO], ZERO)),
                pl.BlockSpec((ONE, 8, rows), lambda j, g, t, sc: (g, ZERO, ZERO)),
                pl.BlockSpec((8, rows), lambda j, g, t, sc: (ZERO, ZERO)),
                pl.BlockSpec((8, rows), lambda j, g, t, sc: (ZERO, ZERO)),
            ] + weights,
            out_specs=[
                pl.BlockSpec((TWO, ONE, LANES, FF_HALF), lambda j, g, t, sc: (ZERO, j, ZERO, ZERO)),
                pl.BlockSpec((TWO, ONE, LANES, FF_HALF), lambda j, g, t, sc: (ZERO, j, ZERO, ZERO)),
                pl.BlockSpec((ONE, LANES, FF_HALF), lambda j, g, t, sc: (j, ZERO, ZERO)),
                pl.BlockSpec((ONE, LANES, FF_HALF), lambda j, g, t, sc: (j, ZERO, ZERO)),
                pl.BlockSpec((ONE, 448, WIDTH), lambda j, g, t, sc: (j, ZERO, ZERO)),
                pl.BlockSpec((ONE, 448, WIDTH), lambda j, g, t, sc: (j, ZERO, ZERO)),
            ],
            scratch_shapes=EXPERT_SCRATCH + [pltpu.VMEM((TWO, rows, TWO * width), BF16), pltpu.VMEM((TWO, 8, rows), F32), pltpu.VMEM((WIDTH, FF_HALF), F32)],
        ),
        out_shape=[
            jax.ShapeDtypeStruct((TWO, 4, LANES, FF_HALF), F32),
            jax.ShapeDtypeStruct((TWO, 4, LANES, FF_HALF), F32),
            jax.ShapeDtypeStruct((4, LANES, FF_HALF), F32),
            jax.ShapeDtypeStruct((4, LANES, FF_HALF), F32),
            jax.ShapeDtypeStruct((4, 448, WIDTH), F32),
            jax.ShapeDtypeStruct((4, 448, WIDTH), F32),
        ],
        compiler_params=params(3),
        cost_estimate=pl.CostEstimate(flops=30_000_000_000, bytes_accessed=50_000_000, transcendentals=4_000_000),
    )(sc, b_own, b_other, d_all, d_all, ranks, comb_own, comb_other, w_gate, w_up, *pieces, w_down, wd1)


HEAD_COLS = 8192
HEAD_BLOCK = 1024
HEAD_TILE = 1024
HEAD_HALF = 16000
HEAD_SHIFT = 7808
HEAD_OVERLAP = HEAD_COLS - HEAD_SHIFT


def head_start(x, core):
    return x * HEAD_HALF + core * HEAD_SHIFT


def fill_head_weights(sc, own, p1, rx2, ry2, rx3, ry3, w):
    rep = sc[TWO]
    w[ZERO:LANES, :] = own[ALL]
    w[LANES:256, :] = p1[ALL]
    for k, (rx, ry) in ((TWO, (rx2, ry2)), (3, (rx3, ry3))):
        w[pl.ds(pl.multiple_of(k * LANES + rep * 64, 64), 64), :] = rx[ALL]
        w[pl.ds(pl.multiple_of(k * LANES + (ONE - rep) * 64, 64), 64), :] = ry[ALL]


def head_weight_specs():
    return [pl.BlockSpec((LANES, HEAD_BLOCK), lambda i, sc: (ZERO, i))] * TWO + [pl.BlockSpec((64, HEAD_BLOCK), lambda i, sc: (ZERO, i))] * 4


def head_stats_kernel(sc, x_ref, own, p1, rx2, ry2, rx3, ry3, out_ref, w, xp, m_acc, s_acc):
    i = pl.program_id(ZERO)
    rows = x_ref.shape[ZERO]

    @pl.when(i == ZERO)
    def _():
        xp[ALL] = permuted_columns(x_ref, sc[3])
        m_acc[ALL] = jnp.full((rows, LANES), -1e30, F32)
        s_acc[ALL] = jnp.zeros((rows, LANES), F32)

    fill_head_weights(sc, own, p1, rx2, ry2, rx3, ry3, w)
    first_new = jnp.where((sc[ZERO] == ONE) & (i == ZERO), HEAD_OVERLAP, ZERO)
    tiles = [slice(t, t + HEAD_TILE) for t in range(ZERO, rows, HEAD_TILE)]

    def update(tile, logits):
        pieces = []
        for q in range(HEAD_BLOCK // LANES):
            piece = logits[:, q * LANES:(q + ONE) * LANES]
            if q * LANES < HEAD_OVERLAP:
                piece = piece + jnp.where(q * LANES >= first_new, 0.0, -1e30)
            pieces.append(piece)
        peak = m_acc[tile, :]
        top = functools.reduce(jnp.maximum, pieces, peak)
        total = s_acc[tile, :] * jnp.exp(peak - top)
        for piece in pieces:
            total = total + jnp.exp(piece - top)
        m_acc[tile, :] = top
        s_acc[tile, :] = total

    ahead = dot_nn(xp[tiles[ZERO], :], w[ALL])
    for n, tile in enumerate(tiles):
        logits = ahead
        if n + ONE < len(tiles):
            ahead = dot_nn(xp[tiles[n + ONE], :], w[ALL])
        update(tile, logits)

    @pl.when(i == pl.num_programs(ZERO) - ONE)
    def _():
        top = m_acc[ALL]
        highest = jnp.max(top, axis=ONE, keepdims=True)
        out_ref[:, ZERO:ONE] = highest
        out_ref[:, ONE:TWO] = jnp.sum(s_acc[ALL] * jnp.exp(top - highest), axis=ONE, keepdims=True)


def head_stats(sc, x_rows, pieces):
    rows, width = x_rows.shape
    return pl.pallas_call(
        head_stats_kernel,
        grid_spec=pltpu.PrefetchScalarGridSpec(
            num_scalar_prefetch=ONE,
            grid=(HEAD_COLS // HEAD_BLOCK,),
            in_specs=[pl.BlockSpec((rows, width), lambda i, sc: (ZERO, ZERO))] + head_weight_specs(),
            out_specs=pl.BlockSpec((rows, 8), lambda i, sc: (ZERO, ZERO)),
            scratch_shapes=[pltpu.VMEM((width, HEAD_BLOCK), BF16), pltpu.VMEM((rows, width), BF16)] + [pltpu.VMEM((rows, LANES), F32)] * TWO,
        ),
        out_shape=jax.ShapeDtypeStruct((rows, 8), F32),
        compiler_params=params(ONE),
        cost_estimate=pl.CostEstimate(flops=17_000_000_000, bytes_accessed=25_000_000, transcendentals=16_800_000),
    )(sc, x_rows, *pieces)


def head_dx_kernel(sc, x_ref, label_ref, lse_ref, own, p1, rx2, ry2, rx3, ry3, dl_ref, dx_ref, picked_ref, w, xp, dx_acc, picked_acc):
    i = pl.program_id(ZERO)
    core, x, rep, me = sc[ZERO], sc[ONE], sc[TWO], sc[3]
    rows = x_ref.shape[ZERO]
    half = rows // TWO

    @pl.when(i == ZERO)
    def _():
        xp[ALL] = permuted_columns(x_ref, me)
        dx_acc[ALL] = jnp.zeros_like(dx_acc)
        picked_acc[ALL] = jnp.zeros_like(picked_acc)

    fill_head_weights(sc, own, p1, rx2, ry2, rx3, ry3, w)
    start = head_start(x, core) + i * HEAD_BLOCK
    first_new = jnp.where((core == ONE) & (i == ZERO), HEAD_OVERLAP, ZERO)
    cols = lax.broadcasted_iota(jnp.int32, (HEAD_TILE, HEAD_BLOCK), ONE)
    count = half // HEAD_TILE
    tiles = []
    for side in (rep, ONE - rep):
        for t in range(count):
            tiles.append(pl.ds(pl.multiple_of(side * half + t * HEAD_TILE, HEAD_TILE), HEAD_TILE))

    def gradient(tile, logits):
        hit = cols == label_ref[tile, :] - start
        prob = jnp.exp(logits - lse_ref[tile, :])
        picked = jnp.where(hit, logits, 0.0)
        picked_acc[ALL] += sum(jnp.where(q * LANES >= first_new, 1.0, 0.0) * jnp.sum(picked[:, q * LANES:(q + ONE) * LANES].reshape(HEAD_TILE // 8, 8, LANES), axis=ZERO)
                               for q in range(HEAD_BLOCK // LANES))
        d_logits = (jnp.where(hit, prob - 1.0, prob) * (1.0 / rows)).astype(BF16)
        dl_ref[tile, :] = d_logits
        return d_logits

    def project(n, d_logits):
        overlap = d_logits[:, ZERO:HEAD_OVERLAP]
        overlap = jnp.where(first_new == ZERO, overlap.astype(F32), 0.0).astype(BF16)
        masked = jnp.concatenate([overlap, d_logits[:, HEAD_OVERLAP:]], axis=ONE)
        dx_acc[n * HEAD_TILE:(n + ONE) * HEAD_TILE, :] += dot_nt(masked, w[ALL])

    ahead = dot_nn(xp[tiles[ZERO], :], w[ALL])
    for n, tile in enumerate(tiles):
        logits = ahead
        if n + ONE < len(tiles):
            ahead = dot_nn(xp[tiles[n + ONE], :], w[ALL])
        d_logits = gradient(tile, logits)
        if n < count:
            project(n, d_logits)

    @pl.when(i == pl.num_programs(ZERO) - ONE)
    def _():
        for k in range(4):
            dx_ref[:, pl.ds(pl.multiple_of((me ^ k) * LANES, LANES), LANES)] = dx_acc[:, k * LANES:(k + ONE) * LANES]
        picked_ref[ALL] = picked_acc[ALL]


def head_dx(sc, x_rows, labels, lse, pieces):
    rows, width = x_rows.shape
    return pl.pallas_call(
        head_dx_kernel,
        grid_spec=pltpu.PrefetchScalarGridSpec(
            num_scalar_prefetch=ONE,
            grid=(HEAD_COLS // HEAD_BLOCK,),
            in_specs=[
                pl.BlockSpec((rows, width), lambda i, sc: (ZERO, ZERO)),
                pl.BlockSpec((rows, ONE), lambda i, sc: (ZERO, ZERO)),
                pl.BlockSpec((rows, ONE), lambda i, sc: (ZERO, ZERO)),
            ] + head_weight_specs(),
            out_specs=[pl.BlockSpec((rows, HEAD_BLOCK), lambda i, sc: (ZERO, i)), pl.BlockSpec((rows // TWO, width), lambda i, sc: (ZERO, ZERO)),
                       pl.BlockSpec((8, LANES), lambda i, sc: (ZERO, ZERO))],
            scratch_shapes=[pltpu.VMEM((width, HEAD_BLOCK), BF16), pltpu.VMEM((rows, width), BF16), pltpu.VMEM((rows // TWO, width), F32),
                            pltpu.VMEM((8, LANES), F32)],
        ),
        out_shape=[jax.ShapeDtypeStruct((rows, HEAD_COLS), BF16), jax.ShapeDtypeStruct((rows // TWO, width), F32), jax.ShapeDtypeStruct((8, LANES), F32)],
        compiler_params=params(ONE),
        cost_estimate=pl.CostEstimate(flops=26_000_000_000, bytes_accessed=60_000_000, transcendentals=16_800_000),
    )(sc, x_rows, labels, lse, *pieces)


def head_dw_kernel(sc, xt_ref, dl_ref, d0, d1, d2, d3, xt):
    @pl.when(pl.program_id(ZERO) == ZERO)
    def _():
        me, rep = sc[3], sc[TWO]
        for k in range(TWO):
            xt[k * LANES:(k + ONE) * LANES, :] = xt_ref[pl.ds(pl.multiple_of((me ^ k) * LANES, LANES), LANES), :]
        for k in range(TWO, 4):
            xt[LANES + k * 64:192 + k * 64, :] = xt_ref[pl.ds(pl.multiple_of((me ^ k) * LANES + rep * 64, 64), 64), :]

    dw = dot_nn(xt[ALL], dl_ref[ALL])
    d0[ALL] = dw[ZERO:LANES]
    d1[ALL] = dw[LANES:256]
    d2[ALL] = dw[256:320]
    d3[ALL] = dw[320:384]


def head_dw(sc, x_cols, dl):
    width, rows = x_cols.shape
    block = WIDTH
    return pl.pallas_call(
        head_dw_kernel,
        grid_spec=pltpu.PrefetchScalarGridSpec(
            num_scalar_prefetch=ONE,
            grid=(HEAD_COLS // block,),
            in_specs=[
                pl.BlockSpec((width, rows), lambda i, sc: (ZERO, ZERO)),
                pl.BlockSpec((rows, block), lambda i, sc: (ZERO, i)),
            ],
            out_specs=[pl.BlockSpec((LANES, block), lambda i, sc: (ZERO, i))] * TWO + [pl.BlockSpec((64, block), lambda i, sc: (ZERO, i))] * TWO,
            scratch_shapes=[pltpu.VMEM((384, rows), BF16)],
        ),
        out_shape=[jax.ShapeDtypeStruct((LANES, HEAD_COLS), F32)] * TWO + [jax.ShapeDtypeStruct((64, HEAD_COLS), F32)] * TWO,
        compiler_params=params(ONE),
        cost_estimate=pl.CostEstimate(flops=13_000_000_000, bytes_accessed=52_000_000, transcendentals=ZERO),
    )(sc, x_cols, dl)


def update_near_kernel(sc, rate, w_ref, own, p1, *rest):
    out_ref = rest[-ONE]

    @pl.when(pl.program_id(ZERO) == ZERO)
    def _():
        out_ref[ZERO, :, ZERO] = w_ref[ZERO, :, ZERO] - rate[ZERO] * own[ZERO]

    @pl.when(pl.program_id(ZERO) == ONE)
    def _():
        out_ref[ZERO, :, ZERO] = w_ref[ZERO, :, ZERO] - rate[ZERO] * p1[ZERO]


def update_far_kernel(sc, rate, w_ref, first2, first3, second2, second3, *rest):
    out_ref = rest[-ONE]

    @pl.when((pl.program_id(ZERO) == ZERO) & (sc[TWO] == sc[4]))
    def _():
        out_ref[ZERO, :, ZERO] = w_ref[ZERO, :, ZERO] - rate[ZERO] * first2[ALL]

    @pl.when((pl.program_id(ZERO) == ZERO) & (sc[TWO] != sc[4]))
    def _():
        out_ref[ZERO, :, ZERO] = w_ref[ZERO, :, ZERO] - rate[ZERO] * second2[ALL]

    @pl.when((pl.program_id(ZERO) == ONE) & (sc[TWO] == sc[4]))
    def _():
        out_ref[ZERO, :, ZERO] = w_ref[ZERO, :, ZERO] - rate[ZERO] * first3[ALL]

    @pl.when((pl.program_id(ZERO) == ONE) & (sc[TWO] != sc[4]))
    def _():
        out_ref[ZERO, :, ZERO] = w_ref[ZERO, :, ZERO] - rate[ZERO] * second3[ALL]


def update_blocks(kernel, sc, rate, layer, near, w, grads, grad_specs, previous):
    shape = w.shape
    paired = (shape[ZERO], 4, TWO) + shape[TWO:]

    def whole(s, j, sc):
        return layer, j, jnp.where(s == ZERO, sc[ZERO], ONE - sc[ZERO]), ZERO, (sc[ONE] if near else ONE - sc[ONE])

    block = pl.BlockSpec((ONE, TWO, ONE, LANES, FF_HALF), whole)
    in_specs = [pl.BlockSpec(memory_space=pltpu.SMEM), block] + grad_specs
    args = [sc, rate, w.reshape(paired)] + grads
    aliases = {}
    if previous is not None:
        in_specs.append(pl.BlockSpec(memory_space=pl.ANY))
        aliases = {len(args): ZERO}
        args.append(previous.reshape(paired))
    return pl.pallas_call(
        kernel,
        grid_spec=pltpu.PrefetchScalarGridSpec(num_scalar_prefetch=ONE, grid=(TWO, TWO), in_specs=in_specs, out_specs=block),
        out_shape=jax.ShapeDtypeStruct(paired, F32),
        input_output_aliases=aliases,
        compiler_params=params(TWO),
        cost_estimate=pl.CostEstimate(flops=2_000_000, bytes_accessed=11_000_000, transcendentals=ZERO),
    )(*args).reshape(shape)


def early(s, j):
    return jnp.where(s == ZERO, j, ONE)


def late(s, j):
    return jnp.where(s == ZERO, ZERO, j)


def update_near(sc, rate, layer, matrix, w, own, p1, previous=None):
    specs = [
        pl.BlockSpec((ONE, TWO, LANES, FF_HALF), lambda s, j, sc: (matrix, early(s, j), ZERO, ZERO)),
        pl.BlockSpec((ONE, TWO, LANES, FF_HALF), lambda s, j, sc: (matrix, late(s, j), ZERO, ZERO)),
    ]
    return update_blocks(update_near_kernel, sc, rate, layer, True, w, [own, p1], specs, previous)


def update_far(sc, rate, layer, matrix, w, rx2, ry2, rx3, ry3, previous):
    sc = jnp.concatenate([sc, jnp.full((ONE,), matrix, jnp.int32)])

    def spec(place, by_x):
        def index(s, j, sc):
            return jnp.where((sc[TWO] == sc[4]) == by_x, place(s, j), ZERO), ZERO, ZERO

        return pl.BlockSpec((TWO, LANES, FF_HALF), index)

    specs = [spec(early, True), spec(late, True), spec(early, False), spec(late, False)]
    return update_blocks(update_far_kernel, sc, rate, layer, False, w, [rx2, rx3, ry2, ry3], specs, previous)


def update_down_kernel(sc, rate, w_ref, own, p1, *rest):
    out_ref = rest[-ONE]
    s = pl.program_id(ZERO)

    @pl.when(s == ZERO)
    def _():
        out_ref[ZERO, :, ZERO] = w_ref[ZERO, :, ZERO] - rate[ZERO] * own[ALL]

    @pl.when(s == ONE)
    def _():
        out_ref[ZERO, :, ZERO] = w_ref[ZERO, :, ZERO] - rate[ZERO] * p1[ALL]


def update_down(sc, rate, layer, w, own, p1, previous=None):
    shape = w.shape
    paired = (shape[ZERO], 4, TWO) + shape[TWO:]
    whole = lambda s, j, sc: (layer, j, jnp.where(s == ZERO, sc[ZERO], ONE - sc[ZERO]), ZERO, ZERO)
    in_specs = [
        pl.BlockSpec(memory_space=pltpu.SMEM),
        pl.BlockSpec((ONE, TWO, ONE, 448, WIDTH), whole),
        pl.BlockSpec((TWO, 448, WIDTH), lambda s, j, sc: (early(s, j), ZERO, ZERO)),
        pl.BlockSpec((TWO, 448, WIDTH), lambda s, j, sc: (late(s, j), ZERO, ZERO)),
    ]
    args = [sc, rate, w.reshape(paired), own, p1]
    aliases = {}
    if previous is not None:
        in_specs.append(pl.BlockSpec(memory_space=pl.ANY))
        aliases = {len(args): ZERO}
        args.append(previous.reshape(paired))
    return pl.pallas_call(
        update_down_kernel,
        grid_spec=pltpu.PrefetchScalarGridSpec(
            num_scalar_prefetch=ONE, grid=(TWO, TWO), in_specs=in_specs, out_specs=pl.BlockSpec((ONE, TWO, ONE, 448, WIDTH), whole),
        ),
        out_shape=jax.ShapeDtypeStruct(paired, F32),
        input_output_aliases=aliases,
        compiler_params=params(TWO),
        cost_estimate=pl.CostEstimate(flops=4_000_000, bytes_accessed=22_000_000, transcendentals=ZERO),
    )(*args).reshape(shape)


def update_head_kernel(sc, rate, w_ref, own, p1, rx2, ry2, rx3, ry3, out_ref):
    half = pl.program_id(ZERO) // (pl.num_programs(ZERO) // TWO)
    core, x, rep = sc[ZERO], sc[ONE], sc[TWO]
    lr = rate[ZERO]
    blocks = (
        (x, core, own[ALL]),
        (x, ONE - core, p1[ALL]),
        (ONE - x, core, jnp.where(half == rep, rx2[ALL], ry2[ALL])),
        (ONE - x, ONE - core, jnp.where(half == rep, rx3[ALL], ry3[ALL])),
    )
    for bx, bc, grad in blocks:
        cols = pl.ds(pl.multiple_of(head_start(bx, bc), LANES), HEAD_COLS)
        out_ref[:, cols] = w_ref[:, cols] - lr * grad


def update_head(sc, rate, w, own, p1, rx2, ry2, rx3, ry3):
    rows, vocab = w.shape
    step = 16
    count = rows // step
    inner = count // TWO
    return pl.pallas_call(
        update_head_kernel,
        grid_spec=pltpu.PrefetchScalarGridSpec(
            num_scalar_prefetch=ONE,
            grid=(count,),
            in_specs=[
                pl.BlockSpec(memory_space=pltpu.SMEM),
                pl.BlockSpec((step, vocab), lambda i, sc: (i, ZERO)),
                pl.BlockSpec((step, HEAD_COLS), lambda i, sc: (i, ZERO)),
                pl.BlockSpec((step, HEAD_COLS), lambda i, sc: (i, ZERO)),
            ] + [pl.BlockSpec((step, HEAD_COLS), lambda i, sc: (i % inner, ZERO))] * 4,
            out_specs=pl.BlockSpec((step, vocab), lambda i, sc: (i, ZERO)),
        ),
        out_shape=jax.ShapeDtypeStruct(w.shape, F32),
        compiler_params=params(ONE),
        cost_estimate=pl.CostEstimate(flops=8_000_000, bytes_accessed=50_000_000, transcendentals=ZERO),
    )(sc, rate, w, own, p1, rx2, ry2, rx3, ry3)


def update_embedding_kernel(sc, rate, ids_ref, d_ref, w_ref, out_ref):
    rows = w_ref.shape[ZERO]
    first = sc[3] * (pl.num_programs(ZERO) * rows) + pl.program_id(ZERO) * rows
    index = lax.broadcasted_iota(jnp.int32, (rows, ids_ref.shape[ONE]), ZERO) + first
    onehot = jnp.where(index == ids_ref[ALL], 1.0, 0.0).astype(BF16)
    out_ref[ALL] = w_ref[ALL] - rate[ZERO] * dot_nn(onehot, d_ref[ALL])


def update_embedding(sc, rate, ids, d_rows, w):
    rows, width = w.shape
    step = 800
    tokens = d_rows.shape[ZERO]
    return pl.pallas_call(
        update_embedding_kernel,
        grid_spec=pltpu.PrefetchScalarGridSpec(
            num_scalar_prefetch=ONE,
            grid=(rows // step,),
            in_specs=[
                pl.BlockSpec(memory_space=pltpu.SMEM),
                pl.BlockSpec((ONE, tokens), lambda i, sc: (ZERO, ZERO)),
                pl.BlockSpec((tokens, width), lambda i, sc: (ZERO, ZERO)),
                pl.BlockSpec((step, width), lambda i, sc: (i, ZERO)),
            ],
            out_specs=pl.BlockSpec((step, width), lambda i, sc: (i, ZERO)),
        ),
        out_shape=jax.ShapeDtypeStruct(w.shape, F32),
        compiler_params=params(ONE),
        cost_estimate=pl.CostEstimate(flops=17_000_000_000, bytes_accessed=35_000_000, transcendentals=ZERO),
    )(sc, rate, ids, d_rows, w)


def peer_of(rep, me, other_rep, k):
    across = (me, me + ONE - TWO * (me % TWO), (me + TWO) % 4, 3 - me)[k]
    return (ONE - rep if other_rep else rep), across


def exchange_kernel(both, in_ref, out_ref, send_sem, recv_sem):
    rep, me = lax.axis_index(REP), lax.axis_index(FSDP)
    slot = rep * 4 + me if both else me
    peers = [(other, k) for other in ((False, True) if both else (False,)) for k in range(4) if other or k]
    barrier = pltpu.get_barrier_semaphore()
    for other, k in peers:
        pl.semaphore_signal(barrier, inc=ONE, device_id=peer_of(rep, me, other, k), device_id_type=pl.DeviceIdType.MESH)
    pl.semaphore_wait(barrier, len(peers))
    copies = []
    for n, (other, k) in enumerate(peers):
        copy = pltpu.make_async_remote_copy(
            src_ref=in_ref, dst_ref=out_ref.at[slot], send_sem=send_sem.at[n], recv_sem=recv_sem.at[n],
            device_id=peer_of(rep, me, other, k), device_id_type=pl.DeviceIdType.MESH)
        copy.start()
        copies.append(copy)
    out_ref[slot] = in_ref[ALL]
    for copy in copies:
        copy.wait()


def exchange(value, both, collective_id):
    count = 8 if both else 4
    return pl.pallas_call(
        functools.partial(exchange_kernel, both),
        in_specs=[pl.BlockSpec(memory_space=pltpu.VMEM)],
        out_specs=pl.BlockSpec(memory_space=pltpu.VMEM),
        out_shape=jax.ShapeDtypeStruct((count,) + value.shape, value.dtype),
        scratch_shapes=[pltpu.SemaphoreType.DMA((count - ONE,)), pltpu.SemaphoreType.DMA((count - ONE,))],
        compiler_params=pltpu.CompilerParams(collective_id=collective_id, has_side_effects=True),
        cost_estimate=pl.CostEstimate(flops=1_000_000_000, bytes_accessed=100_000, transcendentals=ZERO),
        name="exchange",
    )(value)


def row_major(value):
    return with_layout_constraint(value, Layout(major_to_minor=(ZERO, ONE)))


def to_peer(value, k):
    return lax.ppermute(value, FSDP, [(i, i ^ k) for i in range(4)])


def to_replica(value):
    return lax.ppermute(value, REP, [(ZERO, ONE), (ONE, ZERO)])


def solution(mesh):
    batch_spec = P((REP, FSDP))
    layer_spec = P(None, FSDP)
    expert_spec = P(None, None, FSDP)
    param_specs = (P(FSDP), layer_spec, layer_spec, layer_spec, layer_spec, layer_spec, layer_spec, layer_spec, expert_spec, expert_spec, expert_spec, P(FSDP), P(FSDP))
    in_specs = (batch_spec, batch_spec, batch_spec, P(None, (REP, FSDP)), P()) + param_specs
    out_specs = param_specs + (P(),)

    def train_step(tok_ids, tok_labels, tok_pos, expert_idx, learn_rate, embedding, w_query, w_key, w_value, w_attn_out, g_attn, g_mlp, w_router, w_gate, w_up, w_down, g_final, w_head):
        me = lax.axis_index(FSDP)
        rep = lax.axis_index(REP)
        core, x = me % TWO, me // TWO
        place = jnp.stack([core, x, rep, me]).astype(jnp.int32)
        rate = learn_rate.reshape(ONE)
        layers = w_query.shape[ZERO]
        length = tok_ids.shape[ONE]
        tokens = 8 * length
        cos_tab, sin_tab = rope_tables(tok_pos[ZERO])

        cos_wide = jnp.concatenate([cos_tab[:, ZERO]] * TWO, axis=ONE)
        sin_wide = jnp.concatenate([-sin_tab[:, ZERO], sin_tab[:, ZERO]], axis=ONE)

        packed = jnp.concatenate([tok_ids, tok_labels, expert_idx[ZERO, ZERO].T, expert_idx[ONE, ZERO].T, tok_ids, tok_labels], axis=ZERO)
        packed = exchange(packed, True, ZERO)
        all_ids, all_labels = packed[:, ZERO].reshape(-ONE), packed[:, ONE].reshape(-ONE, ONE)
        group = tokens // TWO
        chosen_all = [packed[:, TWO + TWO * layer:4 + TWO * layer].transpose(ONE, ZERO, TWO).reshape(TWO, tokens) for layer in range(layers)]
        before = (lax.broadcasted_iota(jnp.int32, (group, group), ZERO) < lax.broadcasted_iota(jnp.int32, (group, group), ONE)).astype(BF16)
        routes = []
        for layer in range(layers):
            experts = lax.broadcasted_iota(jnp.int32, (8, tokens), ZERO)
            mask = ((experts == chosen_all[layer][:ONE]) | (experts == chosen_all[layer][ONE:])).reshape(8, TWO, group).transpose(ONE, ZERO, TWO)
            rank = lax.dot_general(mask.astype(BF16), before, (((TWO,), (ZERO,)), ((), ())), preferred_element_type=F32).astype(jnp.int32)
            rank = jnp.where(mask, rank, -ONE)
            counts = jnp.sum(mask.astype(jnp.int32), axis=TWO).reshape(-ONE)
            routes.append((jnp.concatenate([place, counts]), rank, rank.transpose(ZERO, TWO, ONE)))
        sc = routes[ZERO][ZERO]

        def own_group(values, axis=ZERO):
            return lax.dynamic_slice_in_dim(values, rep * group, group, axis)

        def relay(value, k):
            rx = to_peer(value, k)
            return rx, to_replica(rx)

        def near(value):
            return to_peer(value, ONE)

        def send_experts(layer):
            gu1, mine2, mine3, wd1 = pack_experts(place, layer, w_gate, w_up, w_down)
            pieces = (near(gu1), *relay(mine2, TWO), *relay(mine3, 3))
            return pieces, near(wd1)

        def send_head():
            own, p1, mine2, mine3 = pack_head(place, w_head)
            return [own, near(p1), *relay(mine2, TWO), *relay(mine3, 3)]

        final_col = jnp.stack([g_final, jnp.zeros_like(g_final)])[:, :, None]
        unused = jnp.zeros(g_attn.shape + (1408 - 1291,), F32)
        small = jnp.concatenate([w_query, w_key, w_value, w_attn_out, w_router, g_attn[:, :, None], g_mlp[:, :, None], final_col, unused], axis=TWO)
        whole = []
        for layer in range(layers):
            whole.append(lax.all_gather(small[layer].astype(BF16), FSDP, axis=ZERO, tiled=True))
        cuts = (ZERO, WIDTH, 640, 768, 1280, 1288, 1289, 1290, 1291)

        def small_param(layer, slot):
            value = whole[layer][:, cuts[slot]:cuts[slot + ONE]]
            return value[:, ZERO] if slot >= 5 else value

        def attention_params(layer):
            return whole[layer][:, :cuts[3]], whole[layer][:, cuts[3]:cuts[4]], small_param(layer, 5)

        local = own_group(all_ids) - me * embedding.shape[ZERO]
        owned = (local >= ZERO) & (local < embedding.shape[ZERO])
        rows = jnp.take(embedding, jnp.clip(local, ZERO, embedding.shape[ZERO] - ONE), axis=ZERO)
        rows = jnp.where(owned[:, None], rows, 0.0).astype(BF16)
        residual = row_major(lax.psum_scatter(rows, FSDP, scatter_dimension=ZERO, tiled=True).astype(F32))

        sent = [send_experts(layer) for layer in range(layers)]
        head_pieces = send_head()
        saved = []
        for layer in range(layers):
            w_r, gain_m = small_param(layer, 4), small_param(layer, 6)
            before_attention = residual
            residual = row_major(attention_part(residual, *attention_params(layer), cos_tab=cos_tab, sin_tab=sin_tab))
            after_attention = residual
            b = rms_norm(residual, gain_m)
            b_group = lax.all_gather(row_major(b), FSDP, axis=ZERO, tiled=True)
            b_other = to_replica(b_group)
            comb = combine_weights(router_logits(b_group, w_r), own_group(chosen_all[layer], ONE))
            pieces, wd1 = sent[layer]
            partial = expert_forward(sc, layer, b_group, comb.T, w_gate, w_up, pieces, w_down, wd1)
            residual = row_major(residual + lax.psum_scatter(partial, FSDP, scatter_dimension=ZERO, tiled=True))
            saved.append((before_attention, after_attention, b_group, b_other, comb, w_r))

        others, residual = lax.optimization_barrier(([entry[3] for entry in saved], residual))
        comb_others = []
        for layer in range(layers):
            other = lax.dynamic_slice_in_dim(chosen_all[layer], (ONE - rep) * group, group, ONE)
            comb_others.append(combine_weights(router_logits(others[layer], saved[layer][5]), other))
        final, final_vjp = jax.vjp(rms_norm, residual, small_param(ZERO, 7))
        x_all = lax.all_gather(row_major(final), (REP, FSDP), axis=ZERO, tiled=True)
        stats = head_stats(sc, x_all, head_pieces)
        stats = exchange(stats.T, False, ONE)
        peak = jnp.max(stats[:, ZERO], axis=ZERO)
        lse = peak + jnp.log(jnp.sum(stats[:, ONE] * jnp.exp(stats[:, ZERO] - peak), axis=ZERO))
        dl, dx, picked = head_dx(sc, x_all, all_labels, lse[:, None], head_pieces)
        dh0, dh1, dh2, dh3 = head_dw(sc, x_all.T, dl)
        d_final = row_major(lax.psum_scatter(dx, FSDP, scatter_dimension=ZERO, tiled=True))
        d_residual, d_gain_final = final_vjp(d_final.astype(BF16))
        head_returns = [near(dh1), *relay(dh2, TWO), *relay(dh3, 3)]
        new_head = update_head(sc, rate, w_head, dh0, *head_returns)

        small_grads = [None] * layers
        new_gate = new_up = new_down = None
        for layer in reversed(range(layers)):
            before_attention, after_attention, b_group, _, comb, _ = saved[layer]
            d_all = lax.all_gather(row_major(d_residual), (REP, FSDP), axis=ZERO, tiled=True)
            pieces, wd1 = sent[layer]
            scalars, ranks, rank_cols = routes[layer]
            db = expert_dgrad(scalars, layer, b_group, d_all, ranks, rank_cols, comb, w_gate, w_up, pieces, w_down, wd1)
            own, near1, far2, far3, down_own, down_other = expert_wgrad(scalars, layer, b_group, others[layer], d_all, ranks, comb, comb_others[layer], w_gate, w_up, pieces, w_down, wd1)
            returned = (*relay(far2, TWO), *relay(far3, 3))
            gu1 = near(near1)
            down1 = near(down_other)
            new_gate = update_near(place, rate, layer, ZERO, w_gate, own, gu1, new_gate)
            new_up = update_near(place, rate, layer, ONE, w_up, own, gu1, new_up)
            new_gate = update_far(place, rate, layer, ZERO, w_gate, *returned, new_gate)
            new_up = update_far(place, rate, layer, ONE, w_up, *returned, new_up)
            new_down = update_down(sc, rate, layer, w_down, down_own, down1, previous=new_down)
            db = row_major(lax.psum_scatter(db, FSDP, scatter_dimension=ZERO, tiled=True))
            extra = d_gain_final.astype(F32)[None, :] if layer == ZERO else jnp.full((ONE, d_gain_final.shape[ZERO]), jnp.sum(picked), F32)
            gains = whole[layer][:, cuts[5]:cuts[7]].T
            d_residual, grads = block_backward(before_attention, after_attention, d_residual, db, whole[layer], gains, cos_wide, sin_wide, expert_idx[layer, ZERO], extra)
            small_grads[layer] = lax.psum_scatter(grads, FSDP, scatter_dimension=ZERO, tiled=True)

        d_rows = lax.all_gather(row_major(d_residual.astype(BF16)), (REP, FSDP), axis=ZERO, tiled=True)
        new_embedding = update_embedding(sc, rate, all_ids[None, :], d_rows, embedding)

        small_grad = lax.psum(jnp.stack(small_grads), REP)
        new_small = small - learn_rate * small_grad
        mean_loss = (jnp.sum(lse) - small_grad[ONE, ZERO, 1290] / TWO) / tokens

        def new_param(slot):
            value = new_small[:, :, cuts[slot]:cuts[slot + ONE]]
            return value[:, :, ZERO] if slot >= 5 else value

        return (new_embedding, new_param(ZERO), new_param(ONE), new_param(TWO), new_param(3), new_param(5), new_param(6), new_param(4),
                new_gate, new_up, new_down, new_param(7)[ZERO], new_head, mean_loss)


    return jax.shard_map(train_step, mesh=mesh, in_specs=in_specs, out_specs=out_specs, check_vma=False)
```
